256 devices in a mesh: row: 8 (over y_lo, x), col: 32 (over y_hi, z, core).
Axes of the slice: x: 4, y: 4 (y_hi: 2, y_lo: 2; y = y_hi * 2 + y_lo), z: 8, core: 2. Of those that a mesh axis runs over, the one named last changes fastest.
Arguments:
- density: float32 [256, 256, 256], P('col', 'row'), may hold values from 0.5 to 2
- velocity: float32 [3, 256, 256, 256], P(None, 'col', 'row'), may hold values from -0.6 to 0.6
- pressure: float32 [256, 256, 256], P('col', 'row'), may hold values from 1 to 2
- face_field: float32 [3, 256, 256, 256], P(None, 'col', 'row'), may hold values from -0.6 to 0.6
Outputs:
- new_density: float32 [256, 256, 256], P('col', 'row')
- new_momentum: float32 [3, 256, 256, 256], P(None, 'col', 'row')
- new_energy: float32 [256, 256, 256], P('col', 'row')
- new_face_field: float32 [3, 256, 256, 256], P(None, 'col', 'row')
The draws below stay inside these ranges and needn't reach their ends.
All inputs are finite; a program needn't handle non-finite values.
Results may differ from the reference program's by a relative error of at most 0.0003.
Values sent between devices are 32-bit elements; how exact they have to be, the bound alone decides.
A program may use at most 64 MiB of HBM per device.

```python
import math
import jax
import jax.numpy as jnp
from jax import lax

NX = 256
CZ = 8
NY = 256
NZ = 256
N_COL = 32


def block_levels(key, extent, pieces, least, high):
    def one(axis_at, blocks):
        steps = jax.random.uniform(jax.random.fold_in(jax.random.fold_in(key, 6), axis_at), (blocks,), jnp.float32, least / len(pieces), high / len(pieces))
        return jnp.repeat(jnp.exp(steps), extent[axis_at] // blocks).reshape((-1,) + (1,) * (len(extent) - axis_at - 1))

    factor_of = one(*pieces[0])
    for cut in pieces[1:]:
        factor_of = factor_of * one(*cut)
    return factor_of


def setup_inputs(seed: int = 0) -> dict:
    arg_keys = jax.random.split(jax.random.key(seed), 5)
    return {
        "density": jnp.clip(jnp.exp(math.log(2.0) - 1.3862944 * jax.random.uniform(arg_keys[0], (NZ, NY, NX), jnp.float32) ** block_levels(arg_keys[0], (NZ, NY, NX), ((0, 32), (1, 8)), -0.2, 0.2)), 0.5, 2.0),
        "velocity": jnp.clip(jax.random.uniform(arg_keys[1], (3, NZ, NY, NX), jnp.float32, -0.6, 0.6) * block_levels(arg_keys[1], (3, NZ, NY, NX), ((1, 32), (2, 8)), -0.4, 0.0), -0.6, 0.6),
        "pressure": jnp.clip(1.0 + 1.0 * jax.random.uniform(arg_keys[2], (NZ, NY, NX), jnp.float32) ** block_levels(arg_keys[2], (NZ, NY, NX), ((0, 32), (1, 8)), -0.2, 0.2), 1.0, 2.0),
        "face_field": jnp.clip(jax.random.uniform(arg_keys[3], (3, NZ, NY, NX), jnp.float32, -0.6, 0.6) * block_levels(arg_keys[3], (3, NZ, NY, NX), ((1, 32), (2, 8)), -0.4, 0.0), -0.6, 0.6),
    }


gamma_gas = 5.0 / 3.0
time_step = 0.1
coupling = 3.0

def wave_speed(dens, pres, normal, field_a, field_b):
    sound = gamma_gas * pres / dens
    along_n = normal * normal / dens
    across = (field_a * field_a + field_b * field_b) / dens
    total = sound + along_n + across
    inside = (sound - along_n - across) ** 2 + 4.0 * sound * across
    return jnp.sqrt(0.5 * (total + jnp.sqrt(inside)))

def side_terms(side, normal):
    dens, vel_n, vel_a, vel_b, pres, field_a, field_b = side
    magnetic = 0.5 * (normal * normal + field_a * field_a + field_b * field_b)
    energy = pres / (gamma_gas - 1.0) + 0.5 * dens * (vel_n * vel_n + vel_a * vel_a + vel_b * vel_b) + magnetic
    total_p = pres + magnetic
    dot_vb = vel_n * normal + vel_a * field_a + vel_b * field_b
    conserved = [dens, dens * vel_n, dens * vel_a, dens * vel_b, energy, field_a, field_b]
    flux = [dens * vel_n, dens * vel_n * vel_n + total_p - normal * normal, dens * vel_n * vel_a - normal * field_a, dens * vel_n * vel_b - normal * field_b, (energy + total_p) * vel_n - normal * dot_vb, field_a * vel_n - normal * vel_a, field_b * vel_n - normal * vel_b]
    fast_speed = wave_speed(dens, pres, normal, field_a, field_b)
    return (energy, total_p, dot_vb, conserved, flux, fast_speed)

def star_state(side, normal, energy, total_p, dot_vb, edge, middle, star_p):
    dens, vel_n, vel_a, vel_b, pres, field_a, field_b = side
    relative = edge - vel_n
    mass_rate = dens * relative
    edge_gap = edge - middle
    star_dens = mass_rate / edge_gap
    divisor = mass_rate * edge_gap - normal * normal
    offset = normal * (middle - vel_n) / divisor
    star_va = vel_a - field_a * offset
    star_vb = vel_b - field_b * offset
    factor = (mass_rate * relative - normal * normal) / divisor
    star_fa = field_a * factor
    star_fb = field_b * factor
    star_dot = middle * normal + star_va * star_fa + star_vb * star_fb
    star_energy = (relative * energy - total_p * vel_n + star_p * middle + normal * (dot_vb - star_dot)) / edge_gap
    conserved = [star_dens, star_dens * middle, star_dens * star_va, star_dens * star_vb, star_energy, star_fa, star_fb]
    return (conserved, star_va, star_vb, star_fa, star_fb, star_dot)

def hlld_flux(left, right, normal):
    energy_l, total_l, dot_l, cons_l, flux_l, fast_l = side_terms(left, normal)
    energy_r, total_r, dot_r, cons_r, flux_r, fast_r = side_terms(right, normal)
    fastest = jnp.maximum(fast_l, fast_r)
    slow_edge = jnp.minimum(left[1], right[1]) - fastest
    fast_edge = jnp.maximum(left[1], right[1]) + fastest
    mass_l = left[0] * (slow_edge - left[1])
    mass_r = right[0] * (fast_edge - right[1])
    weight = mass_r - mass_l
    middle = (mass_r * right[1] - mass_l * left[1] - total_r + total_l) / weight
    star_p = (mass_r * total_l - mass_l * total_r + mass_l * mass_r * (right[1] - left[1])) / weight
    star_l, sva_l, svb_l, sfa_l, sfb_l, sdot_l = star_state(left, normal, energy_l, total_l, dot_l, slow_edge, middle, star_p)
    star_r, sva_r, svb_r, sfa_r, sfb_r, sdot_r = star_state(right, normal, energy_r, total_r, dot_r, fast_edge, middle, star_p)
    root_l = jnp.sqrt(star_l[0])
    root_r = jnp.sqrt(star_r[0])
    orient = jnp.sign(normal)
    root_sum = root_l + root_r
    dbl_va = (root_l * sva_l + root_r * sva_r + (sfa_r - sfa_l) * orient) / root_sum
    dbl_vb = (root_l * svb_l + root_r * svb_r + (sfb_r - sfb_l) * orient) / root_sum
    dbl_fa = (root_l * sfa_r + root_r * sfa_l + root_l * root_r * (sva_r - sva_l) * orient) / root_sum
    dbl_fb = (root_l * sfb_r + root_r * sfb_l + root_l * root_r * (svb_r - svb_l) * orient) / root_sum
    dbl_dot = middle * normal + dbl_va * dbl_fa + dbl_vb * dbl_fb
    dbl_energy_l = star_l[4] - root_l * (sdot_l - dbl_dot) * orient
    dbl_energy_r = star_r[4] + root_r * (sdot_r - dbl_dot) * orient
    double_l = [star_l[0], star_l[1], star_l[0] * dbl_va, star_l[0] * dbl_vb, dbl_energy_l, dbl_fa, dbl_fb]
    double_r = [star_r[0], star_r[1], star_r[0] * dbl_va, star_r[0] * dbl_vb, dbl_energy_r, dbl_fa, dbl_fb]
    inner_l = middle - jnp.abs(normal) / root_l
    inner_r = middle + jnp.abs(normal) / root_r
    result = []
    for member in range(7):
        fstar_l = flux_l[member] + slow_edge * (star_l[member] - cons_l[member])
        fdbl_l = fstar_l + inner_l * (double_l[member] - star_l[member])
        fstar_r = flux_r[member] + fast_edge * (star_r[member] - cons_r[member])
        fdbl_r = fstar_r + inner_r * (double_r[member] - star_r[member])
        chosen = jnp.where(fast_edge > 0.0, fstar_r, flux_r[member])
        chosen = jnp.where(inner_r > 0.0, fdbl_r, chosen)
        chosen = jnp.where(middle > 0.0, fdbl_l, chosen)
        chosen = jnp.where(inner_l > 0.0, fstar_l, chosen)
        chosen = jnp.where(slow_edge > 0.0, flux_l[member], chosen)
        result.append(chosen)
    return result

def pull(potential):
    return jnp.stack([-0.5 * (jnp.roll(potential, -1, axis=axis_d) - jnp.roll(potential, 1, axis=axis_d)) for axis_d in (2, 1, 0)])

def advance(dens, velocity, pres, face, accel):
    axes_of = (2, 1, 0)
    tangents = ((1, 2), (2, 0), (0, 1))
    cell_field = [0.5 * (face[comp] + jnp.roll(face[comp], -1, axis=axes_of[comp])) for comp in range(3)]
    flux_all = []
    for direction in range(3):
        axis_d = axes_of[direction]
        first, second = tangents[direction]
        right = (dens, velocity[direction], velocity[first], velocity[second], pres, cell_field[first], cell_field[second])
        left = tuple((jnp.roll(value, 1, axis=axis_d) for value in right))
        flux_all.append(hlld_flux(left, right, face[direction]))

    def difference(member_of):
        total = jnp.zeros_like(dens)
        for direction in range(3):
            term = member_of(direction)
            total = total + (jnp.roll(term, -1, axis=axes_of[direction]) - term)
        return total
    momentum = [dens * velocity[comp] for comp in range(3)]
    energy = pres / (gamma_gas - 1.0) + 0.5 * dens * (velocity[0] ** 2 + velocity[1] ** 2 + velocity[2] ** 2) + 0.5 * (cell_field[0] ** 2 + cell_field[1] ** 2 + cell_field[2] ** 2)
    new_dens = dens - time_step * difference(lambda direction: flux_all[direction][0])
    new_momentum = []
    for comp in range(3):

        def member_of(direction, comp=comp):
            first, second = tangents[direction]
            slot = 1 if comp == direction else 2 if comp == first else 3
            return flux_all[direction][slot]
        new_momentum.append(momentum[comp] - time_step * difference(member_of) + time_step * dens * accel[comp])
    work = momentum[0] * accel[0] + momentum[1] * accel[1] + momentum[2] * accel[2]
    new_energy = energy - time_step * difference(lambda direction: flux_all[direction][4]) + time_step * work
    fx_by, fx_bz = (flux_all[0][5], flux_all[0][6])
    fy_bz, fy_bx = (flux_all[1][5], flux_all[1][6])
    fz_bx, fz_by = (flux_all[2][5], flux_all[2][6])
    edge_z = 0.25 * (-fx_by - jnp.roll(fx_by, 1, axis=1) + fy_bx + jnp.roll(fy_bx, 1, axis=2))
    edge_x = 0.25 * (-fy_bz - jnp.roll(fy_bz, 1, axis=0) + fz_by + jnp.roll(fz_by, 1, axis=1))
    edge_y = 0.25 * (fx_bz + jnp.roll(fx_bz, 1, axis=0) - fz_bx - jnp.roll(fz_bx, 1, axis=2))
    new_bx = face[0] - time_step * (jnp.roll(edge_z, -1, axis=1) - edge_z - (jnp.roll(edge_y, -1, axis=0) - edge_y))
    new_by = face[1] - time_step * (jnp.roll(edge_x, -1, axis=0) - edge_x - (jnp.roll(edge_z, -1, axis=2) - edge_z))
    new_bz = face[2] - time_step * (jnp.roll(edge_y, -1, axis=2) - edge_y - (jnp.roll(edge_x, -1, axis=1) - edge_x))
    return (new_dens, jnp.stack(new_momentum), new_energy, jnp.stack([new_bx, new_by, new_bz]))

def eigen(index, length):
    return 2.0 * jnp.cos(index.astype(jnp.float32) * (2.0 * math.pi / length)) - 2.0

def solve_potential(density):
    spectrum = jnp.fft.fftn(density)
    index_z = jnp.arange(NZ, dtype=jnp.int32)
    index_y = jnp.arange(NY, dtype=jnp.int32)
    index_x = jnp.arange(NX, dtype=jnp.int32)
    total = eigen(index_z, NZ)[:, None, None] + eigen(index_y, NY)[None, :, None] + eigen(index_x, NX)[None, None, :]
    anchor = (index_z[:, None, None] == 0) & (index_y[None, :, None] == 0) & (index_x[None, None, :] == 0)
    factor = jnp.where(anchor, 0.0, coupling / jnp.where(anchor, 1.0, total))
    return jnp.real(jnp.fft.ifftn(spectrum * factor)).astype(jnp.float32)

def reference(density, velocity, pressure, face_field):
    potential = solve_potential(density)
    state = jnp.concatenate([density[None], velocity, pressure[None], face_field, potential[None]], axis=0)
    padded = jnp.concatenate([state[:, -2:], state, state[:, :2]], axis=1)

    def one_block(block):
        piece = lax.dynamic_slice_in_dim(padded, (block * CZ).astype(jnp.int32), CZ + 4, 1)
        accel = pull(piece[8])
        new_dens, new_mom, new_energy, new_face = advance(piece[0], piece[1:4], piece[4], piece[5:8], accel)
        return (new_dens[2:-2], new_mom[:, 2:-2], new_energy[2:-2], new_face[:, 2:-2])
    blocks = lax.map(one_block, jnp.arange(N_COL, dtype=jnp.int32))
    new_density = blocks[0].reshape(NZ, NY, NX)
    new_momentum = jnp.transpose(blocks[1], (1, 0, 2, 3, 4)).reshape(3, NZ, NY, NX)
    new_energy = blocks[2].reshape(NZ, NY, NX)
    new_face_field = jnp.transpose(blocks[3], (1, 0, 2, 3, 4)).reshape(3, NZ, NY, NX)
    return (new_density, new_momentum, new_energy, new_face_field)
```

```python
import functools
import math

import jax
import jax.numpy as jnp
import numpy as np
from jax import lax
from jax.experimental import pallas as pl
from jax.experimental.pallas import tpu as pltpu
from jax.sharding import PartitionSpec as P

gamma_gas = 5.0 / 3.0
time_step = 0.1
coupling = 3.0


def padded_2(x, sides, width):
    for axis, dim in sides:
        size, length = (lax.axis_size(axis), x.shape[dim])
        up = [(i, (i + 1) % size) for i in range(size)]
        down = [(j, i) for i, j in up]
        last = lax.slice_in_dim(x, length - width, length, axis=dim)
        leading = lax.slice_in_dim(x, 0, width, axis=dim)
        before = lax.ppermute(last, axis, up)
        after = lax.ppermute(leading, axis, down)
        x = jnp.concatenate([before, x, after], axis=dim)
    return x


def passed_along(x, axis, by):
    size = lax.axis_size(axis)
    return lax.ppermute(x, axis, [(i, (i + by) % size) for i in range(size)])


def wave_speed(dens, pres, normal, field_a, field_b):
    sound = gamma_gas * pres / dens
    along_n = normal * normal / dens
    across = (field_a * field_a + field_b * field_b) / dens
    total = sound + along_n + across
    inside = (sound - along_n - across) ** 2 + 4.0 * sound * across
    return jnp.sqrt(0.5 * (total + jnp.sqrt(inside)))


def side_terms(side, normal):
    dens, vel_n, vel_a, vel_b, pres, field_a, field_b = side
    magnetic = 0.5 * (normal * normal + field_a * field_a + field_b * field_b)
    energy = (
        pres / (gamma_gas - 1.0)
        + 0.5 * dens * (vel_n * vel_n + vel_a * vel_a + vel_b * vel_b)
        + magnetic
    )
    total_p = pres + magnetic
    dot_vb = vel_n * normal + vel_a * field_a + vel_b * field_b
    conserved = [dens, dens * vel_n, dens * vel_a, dens * vel_b, energy, field_a, field_b]
    flux = [
        dens * vel_n,
        dens * vel_n * vel_n + total_p - normal * normal,
        dens * vel_n * vel_a - normal * field_a,
        dens * vel_n * vel_b - normal * field_b,
        (energy + total_p) * vel_n - normal * dot_vb,
        field_a * vel_n - normal * vel_a,
        field_b * vel_n - normal * vel_b,
    ]
    fast_speed = wave_speed(dens, pres, normal, field_a, field_b)
    return (energy, total_p, dot_vb, conserved, flux, fast_speed)


def star_state(side, normal, energy, total_p, dot_vb, edge, middle, star_p):
    dens, vel_n, vel_a, vel_b, pres, field_a, field_b = side
    relative = edge - vel_n
    mass_rate = dens * relative
    edge_gap = edge - middle
    star_dens = mass_rate / edge_gap
    divisor = mass_rate * edge_gap - normal * normal
    offset = normal * (middle - vel_n) / divisor
    star_va = vel_a - field_a * offset
    star_vb = vel_b - field_b * offset
    factor = (mass_rate * relative - normal * normal) / divisor
    star_fa = field_a * factor
    star_fb = field_b * factor
    star_dot = middle * normal + star_va * star_fa + star_vb * star_fb
    star_energy = (
        relative * energy - total_p * vel_n + star_p * middle + normal * (dot_vb - star_dot)
    ) / edge_gap
    conserved = [
        star_dens,
        star_dens * middle,
        star_dens * star_va,
        star_dens * star_vb,
        star_energy,
        star_fa,
        star_fb,
    ]
    return (conserved, star_va, star_vb, star_fa, star_fb, star_dot)


def hlld_flux(left, right, normal):
    energy_l, total_l, dot_l, cons_l, flux_l, fast_l = side_terms(left, normal)
    energy_r, total_r, dot_r, cons_r, flux_r, fast_r = side_terms(right, normal)
    fastest = jnp.maximum(fast_l, fast_r)
    slow_edge = jnp.minimum(left[1], right[1]) - fastest
    fast_edge = jnp.maximum(left[1], right[1]) + fastest
    mass_l = left[0] * (slow_edge - left[1])
    mass_r = right[0] * (fast_edge - right[1])
    weight = mass_r - mass_l
    middle = (mass_r * right[1] - mass_l * left[1] - total_r + total_l) / weight
    star_p = (mass_r * total_l - mass_l * total_r + mass_l * mass_r * (right[1] - left[1])) / weight
    star_l, sva_l, svb_l, sfa_l, sfb_l, sdot_l = star_state(
        left, normal, energy_l, total_l, dot_l, slow_edge, middle, star_p
    )
    star_r, sva_r, svb_r, sfa_r, sfb_r, sdot_r = star_state(
        right, normal, energy_r, total_r, dot_r, fast_edge, middle, star_p
    )
    root_l = jnp.sqrt(star_l[0])
    root_r = jnp.sqrt(star_r[0])
    orient = jnp.sign(normal)
    root_sum = root_l + root_r
    dbl_va = (root_l * sva_l + root_r * sva_r + (sfa_r - sfa_l) * orient) / root_sum
    dbl_vb = (root_l * svb_l + root_r * svb_r + (sfb_r - sfb_l) * orient) / root_sum
    dbl_fa = (
        root_l * sfa_r + root_r * sfa_l + root_l * root_r * (sva_r - sva_l) * orient
    ) / root_sum
    dbl_fb = (
        root_l * sfb_r + root_r * sfb_l + root_l * root_r * (svb_r - svb_l) * orient
    ) / root_sum
    dbl_dot = middle * normal + dbl_va * dbl_fa + dbl_vb * dbl_fb
    dbl_energy_l = star_l[4] - root_l * (sdot_l - dbl_dot) * orient
    dbl_energy_r = star_r[4] + root_r * (sdot_r - dbl_dot) * orient
    double_l = [
        star_l[0],
        star_l[1],
        star_l[0] * dbl_va,
        star_l[0] * dbl_vb,
        dbl_energy_l,
        dbl_fa,
        dbl_fb,
    ]
    double_r = [
        star_r[0],
        star_r[1],
        star_r[0] * dbl_va,
        star_r[0] * dbl_vb,
        dbl_energy_r,
        dbl_fa,
        dbl_fb,
    ]
    inner_l = middle - jnp.abs(normal) / root_l
    inner_r = middle + jnp.abs(normal) / root_r
    result = []
    for member in range(7):
        fstar_l = flux_l[member] + slow_edge * (star_l[member] - cons_l[member])
        fdbl_l = fstar_l + inner_l * (double_l[member] - star_l[member])
        fstar_r = flux_r[member] + fast_edge * (star_r[member] - cons_r[member])
        fdbl_r = fstar_r + inner_r * (double_r[member] - star_r[member])
        chosen = jnp.where(fast_edge > 0.0, fstar_r, flux_r[member])
        chosen = jnp.where(inner_r > 0.0, fdbl_r, chosen)
        chosen = jnp.where(middle > 0.0, fdbl_l, chosen)
        chosen = jnp.where(inner_l > 0.0, fstar_l, chosen)
        chosen = jnp.where(slow_edge > 0.0, flux_l[member], chosen)
        result.append(chosen)
    return result


def inner_pull(rimmed):
    centre = rimmed[1:-1, 1:-1]
    accel_x = -0.5 * (jnp.roll(centre, -1, axis=2) - jnp.roll(centre, 1, axis=2))
    accel_y = -0.5 * (rimmed[1:-1, 2:] - rimmed[1:-1, :-2])
    accel_z = -0.5 * (rimmed[2:, 1:-1] - rimmed[:-2, 1:-1])
    return (accel_x, accel_y, accel_z)


def advance_window(state_pad, accel):
    size_z = state_pad.shape[1] - 4
    size_y = state_pad.shape[2] - 4
    cells_z = size_z + 3
    cells_y = size_y + 3
    face = state_pad[5:8]
    tangents = ((1, 2), (2, 0), (0, 1))
    face_x = face[0, :cells_z, :cells_y]
    cell_field = [
        0.5 * (face_x + jnp.roll(face_x, -1, axis=2)),
        0.5 * (face[1, :cells_z, :cells_y] + face[1, :cells_z, 1 : cells_y + 1]),
        0.5 * (face[2, :cells_z, :cells_y] + face[2, 1 : cells_z + 1, :cells_y]),
    ]
    dens_c = state_pad[0, :cells_z, :cells_y]
    vel_c = [state_pad[1 + comp, :cells_z, :cells_y] for comp in range(3)]
    pres_c = state_pad[4, :cells_z, :cells_y]
    flux_all = []
    for direction in range(3):
        first, second = tangents[direction]
        cells = (
            dens_c,
            vel_c[direction],
            vel_c[first],
            vel_c[second],
            pres_c,
            cell_field[first],
            cell_field[second],
        )
        right = tuple((value[1:, 1:] for value in cells))
        if direction == 0:
            left = tuple((jnp.roll(value, 1, axis=2) for value in right))
        elif direction == 1:
            left = tuple((value[1:, :-1] for value in cells))
        else:
            left = tuple((value[:-1, 1:] for value in cells))
        flux_all.append(hlld_flux(left, right, face[direction, 1:cells_z, 1:cells_y]))

    def difference(member_of):
        term = member_of(0)[1 : size_z + 1, 1 : size_y + 1]
        total = jnp.roll(term, -1, axis=2) - term
        term = member_of(1)
        total = total + (
            term[1 : size_z + 1, 2 : size_y + 2] - term[1 : size_z + 1, 1 : size_y + 1]
        )
        term = member_of(2)
        total = total + (
            term[2 : size_z + 2, 1 : size_y + 1] - term[1 : size_z + 1, 1 : size_y + 1]
        )
        return total

    dens = state_pad[0, 2 : size_z + 2, 2 : size_y + 2]
    velocity = [state_pad[1 + comp, 2 : size_z + 2, 2 : size_y + 2] for comp in range(3)]
    pres = state_pad[4, 2 : size_z + 2, 2 : size_y + 2]
    field_in = [cell_field[comp][2 : size_z + 2, 2 : size_y + 2] for comp in range(3)]
    face_in = [face[comp, 2 : size_z + 2, 2 : size_y + 2] for comp in range(3)]
    momentum = [dens * velocity[comp] for comp in range(3)]
    energy = (
        pres / (gamma_gas - 1.0)
        + 0.5 * dens * (velocity[0] ** 2 + velocity[1] ** 2 + velocity[2] ** 2)
        + 0.5 * (field_in[0] ** 2 + field_in[1] ** 2 + field_in[2] ** 2)
    )
    new_dens = dens - time_step * difference(lambda direction: flux_all[direction][0])
    new_momentum = []
    for comp in range(3):

        def member_of(direction, comp=comp):
            first, second = tangents[direction]
            slot = 1 if comp == direction else 2 if comp == first else 3
            return flux_all[direction][slot]

        new_momentum.append(
            momentum[comp] - time_step * difference(member_of) + time_step * dens * accel[comp]
        )
    work = momentum[0] * accel[0] + momentum[1] * accel[1] + momentum[2] * accel[2]
    new_energy = (
        energy - time_step * difference(lambda direction: flux_all[direction][4]) + time_step * work
    )
    fx_by, fx_bz = (flux_all[0][5], flux_all[0][6])
    fy_bz, fy_bx = (flux_all[1][5], flux_all[1][6])
    fz_bx, fz_by = (flux_all[2][5], flux_all[2][6])
    edge_z = 0.25 * (
        -fx_by[1:, 1:] - fx_by[1:, :-1] + fy_bx[1:, 1:] + jnp.roll(fy_bx[1:, 1:], 1, axis=2)
    )
    edge_x = 0.25 * (-fy_bz[1:, 1:] - fy_bz[:-1, 1:] + fz_by[1:, 1:] + fz_by[1:, :-1])
    edge_y = 0.25 * (
        fx_bz[1:, 1:] + fx_bz[:-1, 1:] - fz_bx[1:, 1:] - jnp.roll(fz_bx[1:, 1:], 1, axis=2)
    )
    low_z = edge_z[:size_z, :size_y]
    low_x = edge_x[:size_z, :size_y]
    low_y = edge_y[:size_z, :size_y]
    new_bx = face_in[0] - time_step * (edge_z[:size_z, 1:] - low_z - (edge_y[1:, :size_y] - low_y))
    new_by = face_in[1] - time_step * (
        edge_x[1:, :size_y] - low_x - (jnp.roll(low_z, -1, axis=2) - low_z)
    )
    new_bz = face_in[2] - time_step * (
        jnp.roll(low_y, -1, axis=2) - low_y - (edge_x[:size_z, 1:] - low_x)
    )
    return (new_dens, jnp.stack(new_momentum), new_energy, jnp.stack([new_bx, new_by, new_bz]))


def tables(size, chunk):
    index = np.arange(size)
    angle = (index[:, None] * index[None, :] % size) * (2.0 * math.pi / size)
    natural = np.cos(angle) + np.sin(angle)
    order = np.arange(size).reshape(size // chunk, chunk).T.reshape(-1)
    values = 2.0 * np.cos(index * (2.0 * math.pi / size)) - 2.0
    as32 = lambda x: np.ascontiguousarray(x, dtype=np.float32)
    return (as32(natural), as32(natural[:, order]), as32(natural[order, :]), values)


def mm(a, b):
    return lax.dot_general(
        a,
        b,
        (((1,), (0,)), ((), ())),
        precision=lax.Precision.HIGHEST,
        preferred_element_type=jnp.float32,
    )


def exchange_chunks(parts):
    flat = []
    for i in range(4):
        flat.append((parts[i][0], parts[i + 4][0]))
    for i in range(4):
        flat.append((parts[i][1], parts[i + 4][1]))
    rows = parts[0][0].shape[0]
    lane = lax.broadcasted_iota(jnp.int32, (rows, 128), 1)
    for bit, width in ((2, 64), (1, 32)):
        keep = (lane // width) % 2 == 0
        fresh = [None] * 8
        for i in range(8):
            if i & bit:
                continue
            j = i | bit
            low, high = flat[i], flat[j]
            fresh[i] = tuple(
                jnp.where(keep, low[h], pltpu.roll(high[h], width, 1)) for h in range(2)
            )
            fresh[j] = tuple(
                jnp.where(keep, pltpu.roll(low[h], 128 - width, 1), high[h]) for h in range(2)
            )
        flat = fresh
    return flat


def poisson_kernel(rows, cols, dens, nat, perm_c, perm_r, eig_z, eig_y, eig_x, out,
                   send_a, recv_a, send_c, recv_c, send_e, recv_e, send_g, recv_g,
                   sa, ra, sc, rc, se, re, sg, rg):
    row = lax.axis_index("row")
    col = lax.axis_index("col")
    barrier = pltpu.get_barrier_semaphore()

    @pl.loop(1, rows)
    def _(s):
        pl.semaphore_signal(barrier, inc=1, device_id={"row": lax.rem(row + s, rows), "col": col},
                            device_id_type=pl.DeviceIdType.MESH)

    @pl.loop(1, cols)
    def _(s):
        pl.semaphore_signal(barrier, inc=1, device_id={"row": row, "col": lax.rem(col + s, cols)},
                            device_id_type=pl.DeviceIdType.MESH)

    spec = mm(dens[...].reshape(256, 256), nat[...])
    parts = [(spec[32 * z : 32 * z + 32, :128], spec[32 * z : 32 * z + 32, 128:]) for z in range(8)]
    parts = exchange_chunks(parts)
    for r in range(8):
        for h in range(2):
            send_a[r, :, 128 * h : 128 * h + 128] = parts[r][h]
    recv_a[row] = send_a[row]
    pl.semaphore_wait(barrier, rows + cols - 2)

    def row_copy(peer, src, dst, ss, rs, slot):
        return pltpu.make_async_remote_copy(
            src_ref=src.at[peer], dst_ref=dst.at[slot], send_sem=ss.at[peer], recv_sem=rs.at[slot],
            device_id={"row": peer, "col": col}, device_id_type=pl.DeviceIdType.MESH)

    def col_copy(peer, src, dst, ss, rs, slot):
        return pltpu.make_async_remote_copy(
            src_ref=src.at[:, peer], dst_ref=dst.at[:, slot], send_sem=ss.at[peer], recv_sem=rs.at[slot],
            device_id={"row": row, "col": peer}, device_id_type=pl.DeviceIdType.MESH)

    def start_row(src, dst, ss, rs):
        @pl.loop(1, rows)
        def _(s):
            row_copy(lax.rem(row + s, rows), src, dst, ss, rs, row).start()

    def start_col(src, dst, ss, rs):
        @pl.loop(1, cols)
        def _(s):
            col_copy(lax.rem(col + s, cols), src, dst, ss, rs, col).start()

    def wait_row(src, dst, ss, rs):
        @pl.loop(1, rows)
        def _(s):
            peer = lax.rem(row + s, rows)
            row_copy(peer, src, dst, ss, rs, peer).wait_recv()

    def wait_col(src, dst, ss, rs):
        @pl.loop(1, cols)
        def _(s):
            peer = lax.rem(col + s, cols)
            col_copy(peer, src, dst, ss, rs, peer).wait_recv()

    start_row(send_a, recv_a, sa, ra)
    wait_row(send_a, recv_a, sa, ra)
    spec = mm(nat[...], recv_a[...].reshape(256, 256))
    for h in range(2):
        send_c[h] = spec[:, 128 * h : 128 * h + 128].reshape(32, 8, 128)
    recv_c[:, col] = send_c[:, col]
    start_col(send_c, recv_c, sc, rc)
    wait_col(send_c, recv_c, sc, rc)
    parts = [tuple(recv_c.at[h][:, y, :] for h in range(2)) for y in range(8)]
    parts = exchange_chunks(parts)
    full = jnp.concatenate([jnp.concatenate(list(p), axis=1) for p in parts], axis=0)
    full = mm(perm_c[...], full)
    total = eig_z[...] + (eig_y[pl.ds(col, 1), :] + eig_x[pl.ds(row, 1), :])
    kz = lax.broadcasted_iota(jnp.int32, (256, 256), 0)
    lane = lax.broadcasted_iota(jnp.int32, (256, 256), 1)
    anchor = kz + lane + row + col == 0
    full = full * jnp.where(anchor, 0.0, (coupling / 2.0**24) / jnp.where(anchor, 1.0, total))
    full = mm(perm_r[...], full)
    parts = [(full[32 * z : 32 * z + 32, :128], full[32 * z : 32 * z + 32, 128:]) for z in range(8)]
    parts = exchange_chunks(parts)
    for y in range(8):
        for h in range(2):
            send_e[h, :, y, :] = parts[y][h]
    recv_e[:, col] = send_e[:, col]
    start_col(send_e, recv_e, se, re)
    wait_col(send_e, recv_e, se, re)
    full = jnp.concatenate([recv_e[h].reshape(256, 128) for h in range(2)], axis=1)
    full = mm(nat[...], full)
    send_g[...] = full.reshape(8, 32, 256)
    recv_g[row] = send_g[row]
    start_row(send_g, recv_g, sg, rg)
    wait_row(send_g, recv_g, sg, rg)
    parts = [(recv_g[r, :, :128], recv_g[r, :, 128:]) for r in range(8)]
    parts = exchange_chunks(parts)
    full = jnp.concatenate([jnp.concatenate(list(p), axis=1) for p in parts], axis=0)
    out[...] = mm(full, nat[...]).reshape(8, 32, 256)

    @pl.loop(1, rows)
    def _(s):
        peer = lax.rem(row + s, rows)
        row_copy(peer, send_a, recv_a, sa, ra, row).wait_send()
        row_copy(peer, send_g, recv_g, sg, rg, row).wait_send()

    @pl.loop(1, cols)
    def _(s):
        peer = lax.rem(col + s, cols)
        col_copy(peer, send_c, recv_c, sc, rc, col).wait_send()
        col_copy(peer, send_e, recv_e, se, re, col).wait_send()


def solve_potential(density):
    rows = lax.axis_size("row")
    cols = lax.axis_size("col")
    nat, perm_c, perm_r, values = tables(256, 8)
    eig_z = np.ascontiguousarray(np.broadcast_to(values[:, None], (256, 256)), dtype=np.float32)
    eig_y = np.repeat(values.reshape(32, 8), 32, axis=1).astype(np.float32)
    eig_x = np.tile(values.reshape(8, 32), (1, 8)).astype(np.float32)
    dma = pltpu.SemaphoreType.DMA
    vm = pltpu.VMEM
    f = jnp.float32
    return pl.pallas_call(
        functools.partial(poisson_kernel, rows, cols),
        out_shape=jax.ShapeDtypeStruct((8, 32, 256), f),
        in_specs=[pl.BlockSpec(memory_space=vm)] * 7,
        out_specs=pl.BlockSpec(memory_space=vm),
        scratch_shapes=[
            vm((8, 32, 256), f), vm((8, 32, 256), f),
            vm((2, 32, 8, 128), f), vm((2, 32, 8, 128), f),
            vm((2, 32, 8, 128), f), vm((2, 32, 8, 128), f),
            vm((8, 32, 256), f), vm((8, 32, 256), f),
            dma((8,)), dma((8,)), dma((32,)), dma((32,)),
            dma((32,)), dma((32,)), dma((8,)), dma((8,)),
        ],
        compiler_params=pltpu.CompilerParams(collective_id=0, has_side_effects=True),
        name="poisson",
    )(density, jnp.asarray(nat), jnp.asarray(perm_c), jnp.asarray(perm_r), jnp.asarray(eig_z),
      jnp.asarray(eig_y), jnp.asarray(eig_x))


def local(density, velocity, pressure, face_field):
    potential = solve_potential(density)
    state = jnp.concatenate([density[None], velocity, pressure[None], face_field], axis=0)
    padded = padded_2(
        jnp.concatenate([state, potential[None]], axis=0), (("row", 2), ("col", 1)), 1
    )
    extra_y = passed_along(padded[6, :, 2:3, :], "row", -1)
    extra_z = passed_along(padded[7, 2:3, :, :], "col", -1)
    state_pad = jnp.pad(padded[:8], ((0, 0), (1, 1), (1, 1), (0, 0)), mode="edge")
    state_pad = state_pad.at[6, 1:-1, -1:, :].set(extra_y)
    state_pad = state_pad.at[7, -1:, 1:-1, :].set(extra_z)
    accel = inner_pull(padded[8])
    return advance_window(state_pad, accel)


def solution(mesh):
    in_specs = (
        P("col", "row", None),
        P(None, "col", "row", None),
        P("col", "row", None),
        P(None, "col", "row", None),
    )
    out_specs = (
        P("col", "row", None),
        P(None, "col", "row", None),
        P("col", "row", None),
        P(None, "col", "row", None),
    )
    return jax.shard_map(local, mesh=mesh, in_specs=in_specs, out_specs=out_specs, check_vma=False)
```

```python
import functools
import math

import jax
import jax.numpy as jnp
import numpy as np
from jax import lax
from jax.experimental import pallas as pl
from jax.experimental.pallas import tpu as pltpu
from jax.sharding import PartitionSpec as P

gamma_gas = 5.0 / 3.0
time_step = 0.1
coupling = 3.0


def tables(size, chunk):
    index = np.arange(size)
    angle = (index[:, None] * index[None, :] % size) * (2.0 * math.pi / size)
    natural = np.cos(angle) + np.sin(angle)
    order = np.arange(size).reshape(size // chunk, chunk).T.reshape(-1)
    values = 2.0 * np.cos(index * (2.0 * math.pi / size)) - 2.0
    as32 = lambda x: np.ascontiguousarray(x, dtype=np.float32)
    return (as32(natural), as32(natural[:, order]), as32(natural[order, :]), values)


def mm(a, b):
    return lax.dot_general(
        a,
        b,
        (((1,), (0,)), ((), ())),
        precision=lax.Precision.HIGHEST,
        preferred_element_type=jnp.float32,
    )


def exchange_chunks(parts):
    flat = []
    for i in range(4):
        flat.append((parts[i][0], parts[i + 4][0]))
    for i in range(4):
        flat.append((parts[i][1], parts[i + 4][1]))
    rows = parts[0][0].shape[0]
    lane = lax.broadcasted_iota(jnp.int32, (rows, 128), 1)
    for bit, width in ((2, 64), (1, 32)):
        keep = (lane // width) % 2 == 0
        fresh = [None] * 8
        for i in range(8):
            if i & bit:
                continue
            j = i | bit
            low, high = flat[i], flat[j]
            fresh[i] = tuple(
                jnp.where(keep, low[h], pltpu.roll(high[h], width, 1)) for h in range(2)
            )
            fresh[j] = tuple(
                jnp.where(keep, pltpu.roll(low[h], 128 - width, 1), high[h]) for h in range(2)
            )
        flat = fresh
    return flat


def shift_x_down(x):
    return pltpu.roll(x, 1, 1)


def shift_x_up(x):
    return pltpu.roll(x, 255, 1)


def side_terms(side, normal, normal_sq):
    dens, vel_n, vel_a, vel_b, pres, field_a, field_b, inv_dens, sound, hydro = side
    across = field_a * field_a + field_b * field_b
    magnetic = 0.5 * (normal_sq + across)
    energy = hydro + magnetic
    total_p = pres + magnetic
    dot_vb = vel_n * normal + vel_a * field_a + vel_b * field_b
    along = normal_sq * inv_dens
    across = across * inv_dens
    gap = sound - along - across
    fast_sq = sound + along + across + jnp.sqrt(gap * gap + 4.0 * sound * across)
    return (energy, total_p, dot_vb, fast_sq)


def star_state(side, normal, normal_sq, energy, total_p, dot_vb, relative, mass, edge, middle, star_p):
    dens, vel_n, vel_a, vel_b, pres, field_a, field_b = side[:7]
    edge_gap = edge - middle
    inv_gap = 1.0 / edge_gap
    inv_div = 1.0 / (mass * edge_gap - normal_sq)
    star_dens = mass * inv_gap
    offset = normal * (middle - vel_n) * inv_div
    star_va = vel_a - field_a * offset
    star_vb = vel_b - field_b * offset
    factor = (mass * relative - normal_sq) * inv_div
    star_fa = field_a * factor
    star_fb = field_b * factor
    star_dot = middle * normal + star_va * star_fa + star_vb * star_fb
    star_energy = (
        relative * energy - total_p * vel_n + star_p * middle + normal * (dot_vb - star_dot)
    ) * inv_gap
    return (star_dens, star_va, star_vb, star_fa, star_fb, star_dot, star_energy, jnp.sqrt(star_dens))


def hlld_flux(left, right, normal):
    normal_sq = normal * normal
    energy_l, total_l, dot_l, fast_l = side_terms(left, normal, normal_sq)
    energy_r, total_r, dot_r, fast_r = side_terms(right, normal, normal_sq)
    fastest = jnp.sqrt(0.5 * jnp.maximum(fast_l, fast_r))
    slow_edge = jnp.minimum(left[1], right[1]) - fastest
    fast_edge = jnp.maximum(left[1], right[1]) + fastest
    rel_l = slow_edge - left[1]
    rel_r = fast_edge - right[1]
    mass_l = left[0] * rel_l
    mass_r = right[0] * rel_r
    inv_weight = 1.0 / (mass_r - mass_l)
    middle = (mass_r * right[1] - mass_l * left[1] - total_r + total_l) * inv_weight
    star_p = (
        mass_r * total_l - mass_l * total_r + mass_l * mass_r * (right[1] - left[1])
    ) * inv_weight
    star_l = star_state(
        left, normal, normal_sq, energy_l, total_l, dot_l, rel_l, mass_l, slow_edge, middle, star_p
    )
    star_r = star_state(
        right, normal, normal_sq, energy_r, total_r, dot_r, rel_r, mass_r, fast_edge, middle, star_p
    )
    root_l, root_r = star_l[7], star_r[7]
    orient = jnp.where(normal > 0.0, 1.0, jnp.where(normal < 0.0, -1.0, 0.0))
    inv_sum = 1.0 / (root_l + root_r)
    both = root_l * root_r * orient
    dbl_va = (root_l * star_l[1] + root_r * star_r[1] + (star_r[3] - star_l[3]) * orient) * inv_sum
    dbl_vb = (root_l * star_l[2] + root_r * star_r[2] + (star_r[4] - star_l[4]) * orient) * inv_sum
    dbl_fa = (root_l * star_r[3] + root_r * star_l[3] + both * (star_r[1] - star_l[1])) * inv_sum
    dbl_fb = (root_l * star_r[4] + root_r * star_l[4] + both * (star_r[2] - star_l[2])) * inv_sum
    dbl_dot = middle * normal + dbl_va * dbl_fa + dbl_vb * dbl_fb
    on_left = (middle > 0.0) | (slow_edge > 0.0)

    def pick(low, high):
        return jnp.where(on_left, low, high)

    dens, vel_n, vel_a, vel_b = [pick(left[i], right[i]) for i in range(4)]
    field_a, field_b = [pick(left[i], right[i]) for i in (5, 6)]
    energy = pick(energy_l, energy_r)
    total_p = pick(total_l, total_r)
    dot_vb = pick(dot_l, dot_r)
    edge = pick(slow_edge, fast_edge)
    s_dens, s_va, s_vb, s_fa, s_fb, s_dot, s_energy, root = [
        pick(low, high) for low, high in zip(star_l, star_r)
    ]
    way = pick(-1.0, 1.0)
    inner = middle + way * jnp.abs(normal) / root
    ahead = inner > 0.0
    outer = (on_left & (slow_edge > 0.0)) | ~(on_left | (fast_edge > 0.0) | ahead)
    double = (on_left ^ ahead) & ~outer
    d_energy = s_energy + way * root * (s_dot - dbl_dot) * orient
    to_star = jnp.where(outer, 0.0, edge)
    to_double = jnp.where(double, inner, 0.0)
    mass = dens * vel_n
    return (
        mass + to_star * (s_dens - dens),
        mass * vel_n + total_p - normal_sq + to_star * (s_dens * middle - mass),
        mass * vel_a
        - normal * field_a
        + to_star * (s_dens * s_va - dens * vel_a)
        + to_double * (s_dens * (dbl_va - s_va)),
        mass * vel_b
        - normal * field_b
        + to_star * (s_dens * s_vb - dens * vel_b)
        + to_double * (s_dens * (dbl_vb - s_vb)),
        (energy + total_p) * vel_n
        - normal * dot_vb
        + to_star * (s_energy - energy)
        + to_double * (d_energy - s_energy),
        field_a * vel_n - normal * vel_a + to_star * (s_fa - field_a) + to_double * (dbl_fa - s_fa),
        field_b * vel_n - normal * vel_b + to_star * (s_fb - field_b) + to_double * (dbl_fb - s_fb),
    )


def sublane_is(which):
    return lax.broadcasted_iota(jnp.int32, (8, 256), 0) == which


def row_before(load, base, tile):
    mixed = jnp.where(sublane_is(7), load(base + lax.rem(tile + 4, 5)), load(base + tile))
    return pltpu.roll(mixed, 1, 0)


def row_after(load, base, tile):
    mixed = jnp.where(sublane_is(0), load(base + lax.rem(tile + 1, 5)), load(base + tile))
    return pltpu.roll(mixed, 7, 0)


tangents = ((1, 2), (2, 0), (0, 1))


def cell_pass(state, above, cell, base, tile):
    at = base + tile
    dens = state[0, at]
    vel = [state[1 + c, at] for c in range(3)]
    pres = state[4, at]
    cell[0, at] = 0.5 * (state[5, at] + shift_x_up(state[5, at]))
    cell[1, at] = 0.5 * (state[6, at] + row_after(lambda i: state[6, i], base, tile))
    cell[2, at] = 0.5 * (state[7, at] + above)
    inv_dens = 1.0 / dens
    cell[3, at] = inv_dens
    cell[4, at] = gamma_gas * pres * inv_dens
    cell[5, at] = pres / (gamma_gas - 1.0) + 0.5 * dens * (
        vel[0] * vel[0] + vel[1] * vel[1] + vel[2] * vel[2]
    )


def flux_pass(direction, state, cell, flux, base, tile):
    at = base + tile
    first, second = tangents[direction]
    members = (
        (state, 0),
        (state, 1 + direction),
        (state, 1 + first),
        (state, 1 + second),
        (state, 4),
        (cell, first),
        (cell, second),
        (cell, 3),
        (cell, 4),
        (cell, 5),
    )
    right = [ref[f, at] for ref, f in members]
    if direction == 0:
        left = [shift_x_down(value) for value in right]
    elif direction == 1:
        left = [row_before(lambda i, ref=ref, f=f: ref[f, i], base, tile) for ref, f in members]
    else:
        left = [ref[f, at - 5] for ref, f in members]
    result = hlld_flux(left, right, state[5 + direction, at])
    for member in range(7):
        flux[direction, member, at] = result[member]


def edge_pass(flux, edge, base, tile):
    at = base + tile
    edge[2, at] = 0.25 * (
        flux[1, 6, at]
        + shift_x_down(flux[1, 6, at])
        - flux[0, 5, at]
        - row_before(lambda i: flux[0, 5, i], base, tile)
    )
    edge[0, at] = 0.25 * (
        flux[2, 6, at]
        + row_before(lambda i: flux[2, 6, i], base, tile)
        - flux[1, 5, at]
        - flux[1, 5, at - 5]
    )
    edge[1, at] = 0.25 * (
        flux[0, 6, at] + flux[0, 6, at - 5] - flux[2, 5, at] - shift_x_down(flux[2, 5, at])
    )


def update_pass(state, cell, flux, edge, outs, base, tile, plane):
    new_dens, new_mom, new_energy, new_face = outs
    at = base + tile

    def change(slots):
        low = flux[0, slots[0], at]
        total = shift_x_up(low) - low
        total += row_after(lambda i: flux[1, slots[1], i], base, tile) - flux[1, slots[1], at]
        return total + (flux[2, slots[2], at + 5] - flux[2, slots[2], at])

    dens = state[0, at]
    new_dens[plane, tile] = dens - time_step * change((0, 0, 0))
    slots = ((1, 3, 2), (2, 1, 3), (3, 2, 1))
    for c in range(3):
        new_mom[c, plane, tile] = dens * state[1 + c, at] - time_step * change(slots[c])
    field = [cell[c, at] for c in range(3)]
    energy = cell[5, at] + 0.5 * (field[0] * field[0] + field[1] * field[1] + field[2] * field[2])
    new_energy[plane, tile] = energy - time_step * change((4, 4, 4))
    low = [edge[c, at] for c in range(3)]
    new_face[0, plane, tile] = state[5, at] - time_step * (
        row_after(lambda i: edge[2, i], base, tile) - low[2] - (edge[1, at + 5] - low[1])
    )
    new_face[1, plane, tile] = state[6, at] - time_step * (
        edge[0, at + 5] - low[0] - (shift_x_up(low[2]) - low[2])
    )
    new_face[2, plane, tile] = state[7, at] - time_step * (
        shift_x_up(low[1]) - low[1] - (row_after(lambda i: edge[0, i], base, tile) - low[0])
    )


def pull_pass(state, phi, outs, base, tile, plane):
    new_dens, new_mom, new_energy, new_face = outs
    at = base + tile
    centre = phi[at]
    load = lambda i: phi[i]
    accel = (
        -0.5 * (shift_x_up(centre) - shift_x_down(centre)),
        -0.5 * (row_after(load, base, tile) - row_before(load, base, tile)),
        -0.5 * (phi[at + 5] - phi[at - 5]),
    )
    pulled = time_step * state[0, at]
    work = jnp.zeros_like(centre)
    for c in range(3):
        new_mom[c, plane, tile] += pulled * accel[c]
        work += pulled * state[1 + c, at] * accel[c]
    new_energy[plane, tile] += work


def step_kernel(
    rows, cols, dens, vel, pres, face, nat, perm_c, perm_r, eig_z, eig_y, eig_x,
    new_dens, new_mom, new_energy, new_face,
    send_a, recv_a, send_c, recv_c, send_e, recv_e, send_g, recv_g,
    state, cell, flux, edge, phi, above_bz, rim_out, rim_in, phi_out, phi_in,
    sa, ra, sc, rc, se, re, sg, rg, halo_s, halo_r,
):
    row = lax.axis_index("row")
    col = lax.axis_index("col")
    outs = (new_dens, new_mom, new_energy, new_face)
    barrier = pltpu.get_barrier_semaphore()
    row_up = lax.rem(row + 1, rows)
    row_down = lax.rem(row + rows - 1, rows)
    col_up = lax.rem(col + 1, cols)
    col_down = lax.rem(col + cols - 1, cols)

    def copy(src, dst, send, recv, to_row, to_col):
        return pltpu.make_async_remote_copy(
            src_ref=src, dst_ref=dst, send_sem=send, recv_sem=recv,
            device_id={"row": to_row, "col": to_col}, device_id_type=pl.DeviceIdType.MESH,
        )

    def signal(to_row, to_col):
        pl.semaphore_signal(
            barrier, inc=1, device_id={"row": to_row, "col": to_col},
            device_id_type=pl.DeviceIdType.MESH,
        )

    @pl.loop(1, rows)
    def _(s):
        signal(lax.rem(row + s, rows), col)

    @pl.loop(1, cols)
    def _(s):
        signal(row, lax.rem(col + s, cols))

    def row_copy(peer, src, dst, ss, rs, slot):
        return copy(src.at[peer], dst.at[slot], ss.at[peer], rs.at[slot], peer, col)

    def col_copy(peer, src, dst, ss, rs, slot):
        return copy(src.at[:, peer], dst.at[:, slot], ss.at[peer], rs.at[slot], row, peer)

    def start_row(*refs):
        @pl.loop(1, rows)
        def _(s):
            row_copy(lax.rem(row + s, rows), *refs, row).start()

    def start_col(*refs):
        @pl.loop(1, cols)
        def _(s):
            col_copy(lax.rem(col + s, cols), *refs, col).start()

    def wait_row(*refs):
        @pl.loop(1, rows)
        def _(s):
            peer = lax.rem(row + s, rows)
            row_copy(peer, *refs, peer).wait_recv()

    def wait_col(*refs):
        @pl.loop(1, cols)
        def _(s):
            peer = lax.rem(col + s, cols)
            col_copy(peer, *refs, peer).wait_recv()

    over_a = (send_a, recv_a, sa, ra)
    over_c = (send_c, recv_c, sc, rc)
    over_e = (send_e, recv_e, se, re)
    over_g = (send_g, recv_g, sg, rg)

    def halo(number, src, dst, to_row, to_col):
        return copy(src, dst, halo_s.at[number], halo_r.at[number], to_row, to_col)

    rims = (
        halo(0, rim_out.at[0], rim_in.at[0], row_down, col),
        halo(1, rim_out.at[1], rim_in.at[1], row_up, col),
    )
    layers = []
    for number, (layer, base, to_col) in enumerate(((7, 0, col_up), (0, 45, col_down))):
        at = 2 + 5 * number
        layers += [
            halo(at, dens.at[layer], state.at[0, base : base + 4], row, to_col),
            halo(at + 1, vel.at[:, layer], state.at[1:4, base : base + 4], row, to_col),
            halo(at + 2, pres.at[layer], state.at[4, base : base + 4], row, to_col),
            halo(at + 3, face.at[:, layer], state.at[5:8, base : base + 4], row, to_col),
        ]
    layers.append(halo(6, face.at[2, 1], above_bz.at[0:4], row, col_down))
    corners = (
        halo(11, state.at[:, 44], state.at[:, 4], row, col_up),
        halo(12, state.at[:, 9], state.at[:, 49], row, col_down),
        halo(13, state.at[7, 14], above_bz.at[4], row, col_down),
    )
    phi_rims = (
        halo(14, phi_out.at[0], phi_in.at[0], row_down, col),
        halo(15, phi_out.at[1], phi_in.at[1], row_up, col),
    )
    phi_layers = (
        halo(16, phi.at[40:44], phi.at[0:4], row, col_up),
        halo(17, phi.at[5:9], phi.at[45:49], row, col_down),
    )

    spec = mm(dens[...].reshape(256, 256), nat[...])
    parts = [(spec[32 * z : 32 * z + 32, :128], spec[32 * z : 32 * z + 32, 128:]) for z in range(8)]
    parts = exchange_chunks(parts)
    for r in range(8):
        for h in range(2):
            send_a[r, :, 128 * h : 128 * h + 128] = parts[r][h]
    recv_a[row] = send_a[row]
    for f in range(8):
        source = dens if f == 0 else vel.at[f - 1] if f < 4 else pres if f == 4 else face.at[f - 5]
        rim_out[0, f] = source[:, 0, 0, :]
        rim_out[1, f] = source[:, 3, 7, :]
        for k in range(8):
            state[f, 5 * k + 5 : 5 * k + 9] = source[k]
    rim_out[0, 8] = face[1, :, 0, 1, :]
    rim_out[1, 8] = face[1, :, 0, 1, :]
    pl.semaphore_wait(barrier, rows + cols - 2)

    start_row(*over_a)
    for one in rims:
        one.start()
    for one in layers:
        one.start()
    for one in rims:
        one.wait_recv()
    sub = lax.broadcasted_iota(jnp.int32, (8, 256), 0)
    for f in range(8):
        second = rim_in[0, 8] if f == 6 else rim_in[0, f]
        first = rim_in[0, f]
        last = rim_in[1, f]
        for k in range(8):
            tile = jnp.where(sub == 0, first[k : k + 1], last[k : k + 1])
            if f == 6:
                tile = jnp.where(sub == 1, second[k : k + 1], tile)
            state[f, 5 * k + 9] = tile
    for one in corners:
        one.start()
    wait_row(*over_a)

    spec = mm(nat[...], recv_a[...].reshape(256, 256))
    for h in range(2):
        send_c[h] = spec[:, 128 * h : 128 * h + 128].reshape(32, 8, 128)
    recv_c[:, col] = send_c[:, col]
    start_col(*over_c)
    for one in layers:
        one.wait_recv()
    for one in corners:
        one.wait_recv()

    @pl.loop(0, 9)
    def _(plane):
        @pl.loop(0, 5)
        def _(tile):
            cell_pass(state, state[7, plane * 5 + tile + 5], cell, plane * 5, tile)

    @pl.loop(0, 5)
    def _(tile):
        cell_pass(state, above_bz[tile], cell, 45, tile)

    def fluxes(direction, low, high):
        @pl.loop(low, high)
        def _(plane):
            @pl.loop(0, 5)
            def _(tile):
                flux_pass(direction, state, cell, flux, plane * 5, tile)

    fluxes(0, 0, 10)
    fluxes(1, 0, 4)
    wait_col(*over_c)

    parts = [tuple(recv_c.at[h][:, y, :] for h in range(2)) for y in range(8)]
    parts = exchange_chunks(parts)
    full = jnp.concatenate([jnp.concatenate(list(p), axis=1) for p in parts], axis=0)
    full = mm(perm_c[...], full)
    total = eig_z[...] + (eig_y[pl.ds(col, 1), :] + eig_x[pl.ds(row, 1), :])
    kz = lax.broadcasted_iota(jnp.int32, (256, 256), 0)
    lane = lax.broadcasted_iota(jnp.int32, (256, 256), 1)
    anchor = kz + lane + row + col == 0
    full = full * jnp.where(anchor, 0.0, (coupling / 2.0**24) / jnp.where(anchor, 1.0, total))
    full = mm(perm_r[...], full)
    parts = [(full[32 * z : 32 * z + 32, :128], full[32 * z : 32 * z + 32, 128:]) for z in range(8)]
    parts = exchange_chunks(parts)
    for y in range(8):
        for h in range(2):
            send_e[h, :, y, :] = parts[y][h]
    recv_e[:, col] = send_e[:, col]
    start_col(*over_e)
    fluxes(1, 4, 10)
    fluxes(2, 1, 10)
    wait_col(*over_e)
    full = jnp.concatenate([recv_e[h].reshape(256, 128) for h in range(2)], axis=1)
    full = mm(nat[...], full)
    send_g[...] = full.reshape(8, 32, 256)
    recv_g[row] = send_g[row]
    start_row(*over_g)

    @pl.loop(1, 10)
    def _(plane):
        @pl.loop(0, 5)
        def _(tile):
            edge_pass(flux, edge, plane * 5, tile)

    @pl.loop(0, 8)
    def _(plane):
        @pl.loop(0, 4)
        def _(tile):
            update_pass(state, cell, flux, edge, outs, plane * 5 + 5, tile, plane)

    wait_row(*over_g)
    parts = [(recv_g[r, :, :128], recv_g[r, :, 128:]) for r in range(8)]
    parts = exchange_chunks(parts)
    full = jnp.concatenate([jnp.concatenate(list(p), axis=1) for p in parts], axis=0)
    full = mm(full, nat[...]).reshape(8, 4, 8, 256)
    for k in range(8):
        phi[5 * k + 5 : 5 * k + 9] = full[k]
    phi_out[0] = full[:, 0, 0, :]
    phi_out[1] = full[:, 3, 7, :]
    for one in phi_rims:
        one.start()
    for one in phi_layers:
        one.start()
    for one in phi_rims:
        one.wait_recv()
    for k in range(8):
        phi[5 * k + 9] = jnp.where(sub == 0, phi_in[0, k : k + 1], phi_in[1, k : k + 1])
    for one in phi_layers:
        one.wait_recv()

    @pl.loop(0, 8)
    def _(plane):
        @pl.loop(0, 4)
        def _(tile):
            pull_pass(state, phi, outs, plane * 5 + 5, tile, plane)

    @pl.loop(1, rows)
    def _(s):
        peer = lax.rem(row + s, rows)
        row_copy(peer, *over_a, row).wait_send()
        row_copy(peer, *over_g, row).wait_send()

    @pl.loop(1, cols)
    def _(s):
        peer = lax.rem(col + s, cols)
        col_copy(peer, *over_c, col).wait_send()
        col_copy(peer, *over_e, col).wait_send()

    for one in (*rims, *layers, *corners, *phi_rims, *phi_layers):
        one.wait_send()


def local(density, velocity, pressure, face_field):
    rows = lax.axis_size("row")
    cols = lax.axis_size("col")
    nat, perm_c, perm_r, values = tables(256, 8)
    eig_z = np.ascontiguousarray(np.broadcast_to(values[:, None], (256, 256)), dtype=np.float32)
    eig_y = np.repeat(values.reshape(32, 8), 32, axis=1).astype(np.float32)
    eig_x = np.tile(values.reshape(8, 32), (1, 8)).astype(np.float32)
    dma = pltpu.SemaphoreType.DMA
    vm = pltpu.VMEM
    f = jnp.float32
    block = (8, 4, 8, 256)
    scalar = jax.ShapeDtypeStruct(block, f)
    vector = jax.ShapeDtypeStruct((3, *block), f)
    results = pl.pallas_call(
        functools.partial(step_kernel, rows, cols),
        out_shape=(scalar, vector, scalar, vector),
        in_specs=[pl.BlockSpec(memory_space=vm)] * 10,
        out_specs=(pl.BlockSpec(memory_space=vm),) * 4,
        scratch_shapes=[
            vm((8, 32, 256), f), vm((8, 32, 256), f),
            vm((2, 32, 8, 128), f), vm((2, 32, 8, 128), f),
            vm((2, 32, 8, 128), f), vm((2, 32, 8, 128), f),
            vm((8, 32, 256), f), vm((8, 32, 256), f),
            vm((8, 50, 8, 256), f), vm((6, 50, 8, 256), f),
            vm((3, 7, 50, 8, 256), f), vm((3, 50, 8, 256), f),
            vm((50, 8, 256), f), vm((5, 8, 256), f),
            vm((2, 9, 8, 256), f), vm((2, 9, 8, 256), f),
            vm((2, 8, 256), f), vm((2, 8, 256), f),
            dma((8,)), dma((8,)), dma((32,)), dma((32,)),
            dma((32,)), dma((32,)), dma((8,)), dma((8,)),
            dma((18,)), dma((18,)),
        ],
        compiler_params=pltpu.CompilerParams(collective_id=0, has_side_effects=True, vmem_limit_bytes=60 * 1024 * 1024),
        name="step",
    )(
        density.reshape(block), velocity.reshape(3, *block), pressure.reshape(block),
        face_field.reshape(3, *block), jnp.asarray(nat), jnp.asarray(perm_c), jnp.asarray(perm_r),
        jnp.asarray(eig_z), jnp.asarray(eig_y), jnp.asarray(eig_x),
    )
    return (
        results[0].reshape(density.shape),
        results[1].reshape(velocity.shape),
        results[2].reshape(density.shape),
        results[3].reshape(velocity.shape),
    )


def solution(mesh):
    in_specs = (
        P("col", "row", None),
        P(None, "col", "row", None),
        P("col", "row", None),
        P(None, "col", "row", None),
    )
    out_specs = (
        P("col", "row", None),
        P(None, "col", "row", None),
        P("col", "row", None),
        P(None, "col", "row", None),
    )
    return jax.shard_map(local, mesh=mesh, in_specs=in_specs, out_specs=out_specs, check_vma=False)
```

```python
import functools
import math

import jax
import jax.numpy as jnp
import numpy as np
from jax import lax
from jax.experimental import pallas as pl
from jax.experimental.pallas import tpu as pltpu
from jax.sharding import PartitionSpec as P

gamma_gas = 5.0 / 3.0
time_step = 0.1
coupling = 3.0


def tables(size, chunk):
    index = np.arange(size)
    angle = (index[:, None] * index[None, :] % size) * (2.0 * math.pi / size)
    natural = np.cos(angle) + np.sin(angle)
    order = np.arange(size).reshape(size // chunk, chunk).T.reshape(-1)
    values = 2.0 * np.cos(index * (2.0 * math.pi / size)) - 2.0
    as32 = lambda x: np.ascontiguousarray(x, dtype=np.float32)
    return (as32(natural), as32(natural[:, order]), as32(natural[order, :]), values)


def mm(a, b):
    return lax.dot_general(
        a,
        b,
        (((1,), (0,)), ((), ())),
        precision=lax.Precision.HIGHEST,
        preferred_element_type=jnp.float32,
    )


def exchange_chunks(parts):
    flat = []
    for i in range(4):
        flat.append((parts[i][0], parts[i + 4][0]))
    for i in range(4):
        flat.append((parts[i][1], parts[i + 4][1]))
    rows = parts[0][0].shape[0]
    lane = lax.broadcasted_iota(jnp.int32, (rows, 128), 1)
    for bit, width in ((2, 64), (1, 32)):
        keep = (lane // width) % 2 == 0
        fresh = [None] * 8
        for i in range(8):
            if i & bit:
                continue
            j = i | bit
            low, high = flat[i], flat[j]
            fresh[i] = tuple(
                jnp.where(keep, low[h], pltpu.roll(high[h], width, 1)) for h in range(2)
            )
            fresh[j] = tuple(
                jnp.where(keep, pltpu.roll(low[h], 128 - width, 1), high[h]) for h in range(2)
            )
        flat = fresh
    return flat


def shift_x_down(x):
    return pltpu.roll(x, 1, 1)


def shift_x_up(x):
    return pltpu.roll(x, 255, 1)


def side_terms(side, normal, normal_sq):
    dens, vel_n, vel_a, vel_b, pres, field_a, field_b, inv_dens, sound, hydro = side
    across = field_a * field_a + field_b * field_b
    magnetic = 0.5 * (normal_sq + across)
    energy = hydro + magnetic
    total_p = pres + magnetic
    dot_vb = vel_n * normal + vel_a * field_a + vel_b * field_b
    along = normal_sq * inv_dens
    across = across * inv_dens
    gap = sound - along - across
    fast_sq = sound + along + across + jnp.sqrt(gap * gap + 4.0 * sound * across)
    return (energy, total_p, dot_vb, fast_sq)


def star_state(side, normal, normal_sq, energy, total_p, dot_vb, relative, mass, edge, middle, star_p):
    dens, vel_n, vel_a, vel_b, pres, field_a, field_b = side[:7]
    edge_gap = edge - middle
    inv_gap = 1.0 / edge_gap
    inv_div = 1.0 / (mass * edge_gap - normal_sq)
    star_dens = mass * inv_gap
    offset = normal * (middle - vel_n) * inv_div
    star_va = vel_a - field_a * offset
    star_vb = vel_b - field_b * offset
    factor = (mass * relative - normal_sq) * inv_div
    star_fa = field_a * factor
    star_fb = field_b * factor
    star_dot = middle * normal + star_va * star_fa + star_vb * star_fb
    star_energy = (
        relative * energy - total_p * vel_n + star_p * middle + normal * (dot_vb - star_dot)
    ) * inv_gap
    return (star_dens, star_va, star_vb, star_fa, star_fb, star_dot, star_energy, jnp.sqrt(star_dens))


def hlld_flux(left, right, normal):
    normal_sq = normal * normal
    energy_l, total_l, dot_l, fast_l = side_terms(left, normal, normal_sq)
    energy_r, total_r, dot_r, fast_r = side_terms(right, normal, normal_sq)
    fastest = jnp.sqrt(0.5 * jnp.maximum(fast_l, fast_r))
    slow_edge = jnp.minimum(left[1], right[1]) - fastest
    fast_edge = jnp.maximum(left[1], right[1]) + fastest
    rel_l = slow_edge - left[1]
    rel_r = fast_edge - right[1]
    mass_l = left[0] * rel_l
    mass_r = right[0] * rel_r
    inv_weight = 1.0 / (mass_r - mass_l)
    middle = (mass_r * right[1] - mass_l * left[1] - total_r + total_l) * inv_weight
    star_p = (
        mass_r * total_l - mass_l * total_r + mass_l * mass_r * (right[1] - left[1])
    ) * inv_weight
    star_l = star_state(
        left, normal, normal_sq, energy_l, total_l, dot_l, rel_l, mass_l, slow_edge, middle, star_p
    )
    star_r = star_state(
        right, normal, normal_sq, energy_r, total_r, dot_r, rel_r, mass_r, fast_edge, middle, star_p
    )
    root_l, root_r = star_l[7], star_r[7]
    orient = jnp.where(normal > 0.0, 1.0, jnp.where(normal < 0.0, -1.0, 0.0))
    inv_sum = 1.0 / (root_l + root_r)
    both = root_l * root_r * orient
    dbl_va = (root_l * star_l[1] + root_r * star_r[1] + (star_r[3] - star_l[3]) * orient) * inv_sum
    dbl_vb = (root_l * star_l[2] + root_r * star_r[2] + (star_r[4] - star_l[4]) * orient) * inv_sum
    dbl_fa = (root_l * star_r[3] + root_r * star_l[3] + both * (star_r[1] - star_l[1])) * inv_sum
    dbl_fb = (root_l * star_r[4] + root_r * star_l[4] + both * (star_r[2] - star_l[2])) * inv_sum
    dbl_dot = middle * normal + dbl_va * dbl_fa + dbl_vb * dbl_fb
    on_left = (middle > 0.0) | (slow_edge > 0.0)

    def pick(low, high):
        return jnp.where(on_left, low, high)

    dens, vel_n, vel_a, vel_b = [pick(left[i], right[i]) for i in range(4)]
    field_a, field_b = [pick(left[i], right[i]) for i in (5, 6)]
    energy = pick(energy_l, energy_r)
    total_p = pick(total_l, total_r)
    dot_vb = pick(dot_l, dot_r)
    edge = pick(slow_edge, fast_edge)
    s_dens, s_va, s_vb, s_fa, s_fb, s_dot, s_energy, root = [
        pick(low, high) for low, high in zip(star_l, star_r)
    ]
    way = pick(-1.0, 1.0)
    inner = middle + way * jnp.abs(normal) / root
    ahead = inner > 0.0
    outer = (on_left & (slow_edge > 0.0)) | ~(on_left | (fast_edge > 0.0) | ahead)
    double = (on_left ^ ahead) & ~outer
    d_energy = s_energy + way * root * (s_dot - dbl_dot) * orient
    to_star = jnp.where(outer, 0.0, edge)
    to_double = jnp.where(double, inner, 0.0)
    mass = dens * vel_n
    return (
        mass + to_star * (s_dens - dens),
        mass * vel_n + total_p - normal_sq + to_star * (s_dens * middle - mass),
        mass * vel_a
        - normal * field_a
        + to_star * (s_dens * s_va - dens * vel_a)
        + to_double * (s_dens * (dbl_va - s_va)),
        mass * vel_b
        - normal * field_b
        + to_star * (s_dens * s_vb - dens * vel_b)
        + to_double * (s_dens * (dbl_vb - s_vb)),
        (energy + total_p) * vel_n
        - normal * dot_vb
        + to_star * (s_energy - energy)
        + to_double * (d_energy - s_energy),
        field_a * vel_n - normal * vel_a + to_star * (s_fa - field_a) + to_double * (dbl_fa - s_fa),
        field_b * vel_n - normal * vel_b + to_star * (s_fb - field_b) + to_double * (dbl_fb - s_fb),
    )


def sublane_is(which):
    return lax.broadcasted_iota(jnp.int32, (8, 256), 0) == which


def wrapped(tile, by):
    return (tile + by) % 5 if isinstance(tile, int) else lax.rem(tile + by, 5)


def row_before(load, tile):
    return pltpu.roll(jnp.where(sublane_is(7), load(wrapped(tile, 4)), load(tile)), 1, 0)


def row_after(load, tile):
    return pltpu.roll(jnp.where(sublane_is(0), load(wrapped(tile, 1)), load(tile)), 7, 0)


tangents = ((1, 2), (2, 0), (0, 1))


def cell_pass(state, above, cell, left, plane, tile):
    dens = state[0, plane, tile]
    vel = [state[1 + c, plane, tile] for c in range(3)]
    pres = state[4, plane, tile]
    face = [state[5 + c, plane, tile] for c in range(3)]
    cell[0, plane, tile] = 0.5 * (face[0] + shift_x_up(face[0]))
    field_y = 0.5 * (face[1] + row_after(lambda t: state[6, plane, t], tile))
    field_z = 0.5 * (face[2] + above)
    inv_dens = 1.0 / dens
    sound = gamma_gas * pres * inv_dens
    hydro = pres / (gamma_gas - 1.0) + 0.5 * dens * (
        vel[0] * vel[0] + vel[1] * vel[1] + vel[2] * vel[2]
    )
    for f, value in ((1, field_y), (2, field_z), (3, inv_dens), (4, sound), (5, hydro)):
        cell[f, plane, tile] = value
    members = (dens, *vel, pres, field_y, field_z, inv_dens, sound, hydro)
    for f, value in enumerate(members):
        left[f, plane, tile] = shift_x_down(value)


def flux_pass(direction, state, cell, left_x, flux, plane, tile):
    first, second = tangents[direction]
    members = (
        (state, 0),
        (state, 1 + direction),
        (state, 1 + first),
        (state, 1 + second),
        (state, 4),
        (cell, first),
        (cell, second),
        (cell, 3),
        (cell, 4),
        (cell, 5),
    )
    right = [ref[f, plane, tile] for ref, f in members]
    if direction == 0:
        left = [left_x[f, plane, tile] for f in range(10)]
    elif direction == 1:
        left = [row_before(lambda t, ref=ref, f=f: ref[f, plane, t], tile) for ref, f in members]
    else:
        left = [ref[f, plane - 1, tile] for ref, f in members]
    result = hlld_flux(left, right, state[5 + direction, plane, tile])
    for member in range(7):
        flux[direction, member, plane, tile] = result[member]


def edge_pass(flux, edge, plane, tile):
    flow = flux[1, 6, plane, tile]
    edge[2, plane, tile] = 0.25 * (
        flow
        + shift_x_down(flow)
        - flux[0, 5, plane, tile]
        - row_before(lambda t: flux[0, 5, plane, t], tile)
    )
    edge[0, plane, tile] = 0.25 * (
        flux[2, 6, plane, tile]
        + row_before(lambda t: flux[2, 6, plane, t], tile)
        - flux[1, 5, plane, tile]
        - flux[1, 5, plane - 1, tile]
    )
    flow = flux[2, 5, plane, tile]
    edge[1, plane, tile] = 0.25 * (
        flux[0, 6, plane, tile] + flux[0, 6, plane - 1, tile] - flow - shift_x_down(flow)
    )


def update_pass(state, cell, flux, edge, outs, plane, tile):
    new_dens, new_mom, new_energy, new_face = outs
    own = plane - 1

    def change(slots):
        low = flux[0, slots[0], plane, tile]
        total = shift_x_up(low) - low
        total += row_after(lambda t: flux[1, slots[1], plane, t], tile) - flux[1, slots[1], plane, tile]
        return total + (flux[2, slots[2], plane + 1, tile] - flux[2, slots[2], plane, tile])

    dens = state[0, plane, tile]
    new_dens[own, tile] = dens - time_step * change((0, 0, 0))
    slots = ((1, 3, 2), (2, 1, 3), (3, 2, 1))
    for c in range(3):
        new_mom[c, own, tile] = dens * state[1 + c, plane, tile] - time_step * change(slots[c])
    field = [cell[c, plane, tile] for c in range(3)]
    energy = cell[5, plane, tile] + 0.5 * (
        field[0] * field[0] + field[1] * field[1] + field[2] * field[2]
    )
    new_energy[own, tile] = energy - time_step * change((4, 4, 4))
    low = [edge[c, plane, tile] for c in range(3)]
    above = [edge[c, plane + 1, tile] for c in range(2)]
    new_face[0, own, tile] = state[5, plane, tile] - time_step * (
        row_after(lambda t: edge[2, plane, t], tile) - low[2] - (above[1] - low[1])
    )
    new_face[1, own, tile] = state[6, plane, tile] - time_step * (
        above[0] - low[0] - (shift_x_up(low[2]) - low[2])
    )
    new_face[2, own, tile] = state[7, plane, tile] - time_step * (
        shift_x_up(low[1]) - low[1] - (row_after(lambda t: edge[0, plane, t], tile) - low[0])
    )


def pull_pass(state, phi, outs, plane, tile):
    new_dens, new_mom, new_energy, new_face = outs
    own = plane - 1
    centre = phi[plane, tile]
    load = lambda t: phi[plane, t]
    accel = (
        -0.5 * (shift_x_up(centre) - shift_x_down(centre)),
        -0.5 * (row_after(load, tile) - row_before(load, tile)),
        -0.5 * (phi[plane + 1, tile] - phi[plane - 1, tile]),
    )
    pulled = time_step * state[0, plane, tile]
    work = jnp.zeros_like(centre)
    for c in range(3):
        new_mom[c, own, tile] += pulled * accel[c]
        work += pulled * state[1 + c, plane, tile] * accel[c]
    new_energy[own, tile] += work


def step_kernel(
    rows, cols, dens, vel, pres, face, nat_h, perm_c_h, perm_r_h, eig_z_h, eig_y_h, eig_x_h,
    out_dens, out_mom, out_energy, out_face,
    nat, perm_c, perm_r, eig_z, eig_y, eig_x,
    send_a, recv_a, send_c, recv_c, send_e, recv_e, send_g, recv_g,
    state, cell, left, flux, edge, phi, above_bz, rim_out, rim_in, phi_out, phi_in,
    new_dens, new_mom, new_energy, new_face,
    local_s, over_s, over_r, halo_s, halo_r,
):
    row = lax.axis_index("row")
    col = lax.axis_index("col")
    outs = (new_dens, new_mom, new_energy, new_face)
    barrier = pltpu.get_barrier_semaphore()
    row_up = lax.rem(row + 1, rows)
    row_down = lax.rem(row + rows - 1, rows)
    col_up = lax.rem(col + 1, cols)
    col_down = lax.rem(col + cols - 1, cols)

    def copy(src, dst, send, recv, to_row, to_col):
        return pltpu.make_async_remote_copy(
            src_ref=src, dst_ref=dst, send_sem=send, recv_sem=recv,
            device_id={"row": to_row, "col": to_col}, device_id_type=pl.DeviceIdType.MESH,
        )

    def signal(to_row, to_col):
        pl.semaphore_signal(
            barrier, inc=1, device_id={"row": to_row, "col": to_col},
            device_id_type=pl.DeviceIdType.MESH,
        )

    @pl.loop(1, cols)
    def _(s):
        signal(row, lax.rem(col + s, cols))

    @pl.loop(1, rows)
    def _(s):
        signal(lax.rem(row + s, rows), col)

    reads = [
        pltpu.make_async_copy(src, dst, local_s.at[i])
        for i, (src, dst) in enumerate(
            (
                (dens, state.at[0, 1:9, 0:4]),
                (nat_h, nat),
                (vel, state.at[1:4, 1:9, 0:4]),
                (pres, state.at[4, 1:9, 0:4]),
                (face, state.at[5:8, 1:9, 0:4]),
                (perm_c_h, perm_c),
                (perm_r_h, perm_r),
                (eig_z_h, eig_z),
                (eig_y_h, eig_y),
                (eig_x_h, eig_x),
            )
        )
    ]
    writes = [
        pltpu.make_async_copy(src, dst, local_s.at[i])
        for i, (src, dst) in enumerate(
            (
                (new_dens, out_dens),
                (new_face, out_face),
                (new_mom, out_mom),
                (new_energy, out_energy),
            )
        )
    ]
    for one in reads:
        one.start()

    def row_copy(peer, src, dst, number):
        return copy(src.at[peer], dst.at[row], over_s.at[number], over_r.at[number], peer, col)

    def col_copy(peer, src, dst, number):
        return copy(src.at[:, peer], dst.at[:, col], over_s.at[number], over_r.at[number], row, peer)

    def start_row(*over):
        @pl.loop(1, rows)
        def _(s):
            row_copy(lax.rem(row + s, rows), *over).start()

    def start_col(*over):
        @pl.loop(1, cols)
        def _(s):
            col_copy(lax.rem(col + s, cols), *over).start()

    def all_row(src, dst, number):
        part = slice(0, rows - 1)
        return copy(src.at[part], dst.at[part], over_s.at[number], over_r.at[number], row_up, col)

    def all_col(src, dst, number):
        part = slice(0, cols - 1)
        return copy(src.at[:, part], dst.at[:, part], over_s.at[number], over_r.at[number], row, col_up)

    over_a = (send_a, recv_a, 0)
    over_c = (send_c, recv_c, 1)
    over_e = (send_e, recv_e, 2)
    over_g = (send_g, recv_g, 3)

    def halo(number, src, dst, to_row, to_col):
        return copy(src, dst, halo_s.at[number], halo_r.at[number], to_row, to_col)

    rims = (
        halo(0, rim_out.at[0], rim_in.at[0], row_down, col),
        halo(0, rim_out.at[1], rim_in.at[1], row_up, col),
    )
    rims_all = halo(0, rim_out, rim_in, row_up, col)
    layers = (
        halo(1, state.at[:, 8, 0:4], state.at[:, 0, 0:4], row, col_up),
        halo(2, state.at[:, 1, 0:4], state.at[:, 9, 0:4], row, col_down),
        halo(3, state.at[7, 2, 0:4], above_bz.at[0:4], row, col_down),
    )
    corners = (
        halo(4, state.at[:, 8, 4], state.at[:, 0, 4], row, col_up),
        halo(5, state.at[:, 1, 4], state.at[:, 9, 4], row, col_down),
        halo(6, state.at[7, 2, 4], above_bz.at[4], row, col_down),
    )
    phi_rims = (
        halo(7, phi_out.at[0], phi_in.at[0], row_down, col),
        halo(7, phi_out.at[1], phi_in.at[1], row_up, col),
    )
    phi_rims_all = halo(7, phi_out, phi_in, row_up, col)
    phi_layers = (
        halo(8, phi.at[8, 0:4], phi.at[0, 0:4], row, col_up),
        halo(9, phi.at[1, 0:4], phi.at[9, 0:4], row, col_down),
    )

    def cells(low, high, tiles):
        @pl.loop(low, high)
        def _(plane):
            for tile in tiles:
                cell_pass(state, state[7, plane + 1, tile], cell, left, plane, tile)

    def fluxes(direction, low, high, first, last):
        @pl.loop(low, high)
        def _(plane):
            @pl.loop(first, last)
            def _(tile):
                flux_pass(direction, state, cell, left, flux, plane, tile)

    reads[0].wait()
    reads[1].wait()
    spec = mm(state[0, 1:9, 0:4].reshape(256, 256), nat[...])
    parts = [(spec[32 * z : 32 * z + 32, :128], spec[32 * z : 32 * z + 32, 128:]) for z in range(8)]
    parts = exchange_chunks(parts)
    for r in range(8):
        for h in range(2):
            send_a[r, :, 128 * h : 128 * h + 128] = parts[r][h]
    recv_a[row] = send_a[row]
    for one in reads[2:]:
        one.wait()
    for f in range(8):
        rim_out[0, f] = state[f, 1:9, 0, 0, :]
        rim_out[1, f] = state[f, 1:9, 3, 7, :]
    second = state[6, 1:9, 0, 1, :]
    rim_out[0, 8] = second
    rim_out[1, 8] = second

    cells(1, 8, range(3))
    fluxes(0, 1, 8, 0, 3)
    fluxes(1, 1, 8, 1, 3)
    fluxes(2, 2, 8, 0, 3)
    pl.semaphore_wait(barrier, rows + cols - 2)

    start_row(*over_a)
    for one in rims:
        one.start()
    for one in layers:
        one.start()
    rims_all.wait_recv()
    sub = lax.broadcasted_iota(jnp.int32, (8, 256), 0)
    for f in range(8):
        first = rim_in[0, f]
        last = rim_in[1, f]
        second = rim_in[0, 8]
        for k in range(8):
            tile = jnp.where(sub == 0, first[k : k + 1], last[k : k + 1])
            if f == 6:
                tile = jnp.where(sub == 1, second[k : k + 1], tile)
            state[f, k + 1, 4] = tile
    for one in corners:
        one.start()
    cells(1, 8, range(3, 5))
    fluxes(0, 1, 8, 3, 5)
    fluxes(2, 2, 8, 3, 5)
    all_row(*over_a).wait_recv()

    spec = mm(nat[...], recv_a[...].reshape(256, 256))
    for h in range(2):
        send_c[h] = spec[:, 128 * h : 128 * h + 128].reshape(32, 8, 128)
    recv_c[:, col] = send_c[:, col]
    start_col(*over_c)
    fluxes(1, 1, 8, 3, 5)
    fluxes(1, 1, 8, 0, 1)
    for one in (*layers, *corners):
        one.wait_recv()

    cells(0, 1, range(5))
    cells(8, 9, range(5))
    for tile in range(5):
        cell_pass(state, above_bz[tile], cell, left, 9, tile)
    fluxes(0, 8, 10, 0, 5)
    fluxes(0, 0, 1, 0, 5)
    fluxes(1, 8, 10, 0, 5)
    fluxes(1, 0, 1, 0, 5)
    all_col(*over_c).wait_recv()

    parts = [tuple(recv_c.at[h][:, y, :] for h in range(2)) for y in range(8)]
    parts = exchange_chunks(parts)
    full = jnp.concatenate([jnp.concatenate(list(p), axis=1) for p in parts], axis=0)
    full = mm(perm_c[...], full)
    total = eig_z[...] + (eig_y[pl.ds(col, 1), :] + eig_x[pl.ds(row, 1), :])
    kz = lax.broadcasted_iota(jnp.int32, (256, 256), 0)
    lane = lax.broadcasted_iota(jnp.int32, (256, 256), 1)
    anchor = kz + lane + row + col == 0
    full = full * jnp.where(anchor, 0.0, (coupling / 2.0**24) / jnp.where(anchor, 1.0, total))
    full = mm(perm_r[...], full)
    parts = [(full[32 * z : 32 * z + 32, :128], full[32 * z : 32 * z + 32, 128:]) for z in range(8)]
    parts = exchange_chunks(parts)
    for y in range(8):
        for h in range(2):
            send_e[h, :, y, :] = parts[y][h]
    recv_e[:, col] = send_e[:, col]
    start_col(*over_e)
    fluxes(2, 8, 10, 0, 5)
    fluxes(2, 1, 2, 0, 5)

    @pl.loop(1, 10)
    def _(plane):
        for tile in range(5):
            edge_pass(flux, edge, plane, tile)

    @pl.loop(1, 9)
    def _(plane):
        for tile in range(4):
            update_pass(state, cell, flux, edge, outs, plane, tile)

    for one in writes[:2]:
        one.start()
    all_col(*over_e).wait_recv()
    full = jnp.concatenate([recv_e[h].reshape(256, 128) for h in range(2)], axis=1)
    full = mm(nat[...], full)
    send_g[...] = full.reshape(8, 32, 256)
    recv_g[row] = send_g[row]
    start_row(*over_g)
    all_row(*over_g).wait_recv()
    parts = [(recv_g[r, :, :128], recv_g[r, :, 128:]) for r in range(8)]
    parts = exchange_chunks(parts)
    full = jnp.concatenate([jnp.concatenate(list(p), axis=1) for p in parts], axis=0)
    full = mm(full, nat[...]).reshape(8, 4, 8, 256)
    phi[1:9, 0:4] = full
    phi_out[0] = full[:, 0, 0, :]
    phi_out[1] = full[:, 3, 7, :]
    for one in (*phi_rims, *phi_layers):
        one.start()
    phi_rims_all.wait_recv()
    for k in range(8):
        phi[k + 1, 4] = jnp.where(sub == 0, phi_in[0, k : k + 1], phi_in[1, k : k + 1])

    def pulls(low, high):
        @pl.loop(low, high)
        def _(plane):
            for tile in range(4):
                pull_pass(state, phi, outs, plane, tile)

    pulls(2, 8)
    for one in phi_layers:
        one.wait_recv()
    pulls(1, 2)
    pulls(8, 9)
    for one in writes[2:]:
        one.start()
    all_row(*over_a).wait_send()
    all_row(*over_g).wait_send()
    all_col(*over_c).wait_send()
    all_col(*over_e).wait_send()
    for one in (rims_all, *layers, *corners, phi_rims_all, *phi_layers):
        one.wait_send()
    for one in writes:
        one.wait()


def local(density, velocity, pressure, face_field):
    rows = lax.axis_size("row")
    cols = lax.axis_size("col")
    nat, perm_c, perm_r, values = tables(256, 8)
    eig_z = np.ascontiguousarray(np.broadcast_to(values[:, None], (256, 256)), dtype=np.float32)
    eig_y = np.repeat(values.reshape(32, 8), 32, axis=1).astype(np.float32)
    eig_x = np.tile(values.reshape(8, 32), (1, 8)).astype(np.float32)
    dma = pltpu.SemaphoreType.DMA
    f = jnp.float32
    vm = lambda *shape: pltpu.VMEM(shape, f)
    block = (8, 4, 8, 256)
    scalar = jax.ShapeDtypeStruct(block, f)
    vector = jax.ShapeDtypeStruct((3, *block), f)
    results = pl.pallas_call(
        functools.partial(step_kernel, rows, cols),
        out_shape=(scalar, vector, scalar, vector),
        in_specs=[pl.BlockSpec(memory_space=pl.ANY)] * 10,
        out_specs=(pl.BlockSpec(memory_space=pl.ANY),) * 4,
        scratch_shapes=[
            vm(256, 256), vm(256, 256), vm(256, 256), vm(256, 256), vm(32, 256), vm(8, 256),
            vm(8, 32, 256), vm(8, 32, 256),
            vm(2, 32, 8, 128), vm(2, 32, 8, 128),
            vm(2, 32, 8, 128), vm(2, 32, 8, 128),
            vm(8, 32, 256), vm(8, 32, 256),
            vm(8, 10, 5, 8, 256), vm(6, 10, 5, 8, 256), vm(10, 10, 5, 8, 256),
            vm(3, 7, 10, 5, 8, 256), vm(3, 10, 5, 8, 256),
            vm(10, 5, 8, 256), vm(5, 8, 256),
            vm(2, 9, 8, 256), vm(2, 9, 8, 256),
            vm(2, 8, 256), vm(2, 8, 256),
            vm(*block), vm(3, *block), vm(*block), vm(3, *block),
            dma((10,)), dma((4,)), dma((4,)), dma((10,)), dma((10,)),
        ],
        compiler_params=pltpu.CompilerParams(
            collective_id=0, has_side_effects=True, vmem_limit_bytes=60 * 1024 * 1024
        ),
        name="step",
    )(
        density.reshape(block), velocity.reshape(3, *block), pressure.reshape(block),
        face_field.reshape(3, *block), jnp.asarray(nat), jnp.asarray(perm_c), jnp.asarray(perm_r),
        jnp.asarray(eig_z), jnp.asarray(eig_y), jnp.asarray(eig_x),
    )
    return (
        results[0].reshape(density.shape),
        results[1].reshape(velocity.shape),
        results[2].reshape(density.shape),
        results[3].reshape(velocity.shape),
    )


def solution(mesh):
    in_specs = (
        P("col", "row", None),
        P(None, "col", "row", None),
        P("col", "row", None),
        P(None, "col", "row", None),
    )
    out_specs = (
        P("col", "row", None),
        P(None, "col", "row", None),
        P("col", "row", None),
        P(None, "col", "row", None),
    )
    return jax.shard_map(local, mesh=mesh, in_specs=in_specs, out_specs=out_specs, check_vma=False)
```

```python
import functools
import math

import jax
import jax.numpy as jnp
import numpy as np
from jax import lax
from jax.experimental import pallas as pl
from jax.experimental.pallas import tpu as pltpu
from jax.sharding import PartitionSpec as P

gamma_gas = 5.0 / 3.0
time_step = 0.1
coupling = 3.0


def tables(size, chunk):
    index = np.arange(size)
    angle = (index[:, None] * index[None, :] % size) * (2.0 * math.pi / size)
    natural = np.cos(angle) + np.sin(angle)
    order = np.arange(size).reshape(size // chunk, chunk).T.reshape(-1)
    values = 2.0 * np.cos(index * (2.0 * math.pi / size)) - 2.0
    as32 = lambda x: np.ascontiguousarray(x, dtype=np.float32)
    return (as32(natural), as32(natural[:, order]), as32(natural[order, :]), values)


def mm(a, b):
    return lax.dot_general(
        a,
        b,
        (((1,), (0,)), ((), ())),
        precision=lax.Precision.HIGHEST,
        preferred_element_type=jnp.float32,
    )


def transpose_chunks(parts):
    lane = lax.broadcasted_iota(jnp.int32, parts[0].shape, 1)
    for bit, width in ((2, 64), (1, 32)):
        keep = (lane // width) % 2 == 0
        fresh = [None] * 4
        for i in range(4):
            if i & bit:
                continue
            low, high = parts[i], parts[i | bit]
            fresh[i] = jnp.where(keep, low, pltpu.roll(high, width, 1))
            fresh[i | bit] = jnp.where(keep, pltpu.roll(low, 128 - width, 1), high)
        parts = fresh
    return parts


def side_by_side(low, high):
    return jnp.concatenate([low, high], axis=1)


def shift_x_down(x):
    return pltpu.roll(x, 1, 1)


def shift_x_up(x):
    return pltpu.roll(x, 255, 1)


def side_terms(side, normal, normal_sq):
    dens, vel_n, vel_a, vel_b, pres, field_a, field_b, inv_dens, sound, hydro = side
    across = field_a * field_a + field_b * field_b
    magnetic = 0.5 * (normal_sq + across)
    energy = hydro + magnetic
    total_p = pres + magnetic
    dot_vb = vel_n * normal + vel_a * field_a + vel_b * field_b
    along = normal_sq * inv_dens
    across = across * inv_dens
    gap = sound - along - across
    fast_sq = sound + along + across + jnp.sqrt(gap * gap + 4.0 * sound * across)
    return (energy, total_p, dot_vb, fast_sq)


def star_state(side, normal, normal_sq, energy, total_p, dot_vb, relative, mass, edge, middle, star_p):
    dens, vel_n, vel_a, vel_b, pres, field_a, field_b = side[:7]
    edge_gap = edge - middle
    inv_gap = 1.0 / edge_gap
    inv_div = 1.0 / (mass * edge_gap - normal_sq)
    star_dens = mass * inv_gap
    offset = normal * (middle - vel_n) * inv_div
    star_va = vel_a - field_a * offset
    star_vb = vel_b - field_b * offset
    factor = (mass * relative - normal_sq) * inv_div
    star_fa = field_a * factor
    star_fb = field_b * factor
    star_dot = middle * normal + star_va * star_fa + star_vb * star_fb
    star_energy = (
        relative * energy - total_p * vel_n + star_p * middle + normal * (dot_vb - star_dot)
    ) * inv_gap
    return (star_dens, star_va, star_vb, star_fa, star_fb, star_dot, star_energy, jnp.sqrt(star_dens))


def hlld_flux(left, right, normal):
    normal_sq = normal * normal
    energy_l, total_l, dot_l, fast_l = side_terms(left, normal, normal_sq)
    energy_r, total_r, dot_r, fast_r = side_terms(right, normal, normal_sq)
    fastest = jnp.sqrt(0.5 * jnp.maximum(fast_l, fast_r))
    slow_edge = jnp.minimum(left[1], right[1]) - fastest
    fast_edge = jnp.maximum(left[1], right[1]) + fastest
    rel_l = slow_edge - left[1]
    rel_r = fast_edge - right[1]
    mass_l = left[0] * rel_l
    mass_r = right[0] * rel_r
    inv_weight = 1.0 / (mass_r - mass_l)
    middle = (mass_r * right[1] - mass_l * left[1] - total_r + total_l) * inv_weight
    star_p = (
        mass_r * total_l - mass_l * total_r + mass_l * mass_r * (right[1] - left[1])
    ) * inv_weight
    star_l = star_state(
        left, normal, normal_sq, energy_l, total_l, dot_l, rel_l, mass_l, slow_edge, middle, star_p
    )
    star_r = star_state(
        right, normal, normal_sq, energy_r, total_r, dot_r, rel_r, mass_r, fast_edge, middle, star_p
    )
    root_l, root_r = star_l[7], star_r[7]
    orient = jnp.where(normal > 0.0, 1.0, jnp.where(normal < 0.0, -1.0, 0.0))
    inv_sum = 1.0 / (root_l + root_r)
    both = root_l * root_r * orient
    dbl_va = (root_l * star_l[1] + root_r * star_r[1] + (star_r[3] - star_l[3]) * orient) * inv_sum
    dbl_vb = (root_l * star_l[2] + root_r * star_r[2] + (star_r[4] - star_l[4]) * orient) * inv_sum
    dbl_fa = (root_l * star_r[3] + root_r * star_l[3] + both * (star_r[1] - star_l[1])) * inv_sum
    dbl_fb = (root_l * star_r[4] + root_r * star_l[4] + both * (star_r[2] - star_l[2])) * inv_sum
    dbl_dot = middle * normal + dbl_va * dbl_fa + dbl_vb * dbl_fb
    on_left = (middle > 0.0) | (slow_edge > 0.0)

    def pick(low, high):
        return jnp.where(on_left, low, high)

    dens, vel_n, vel_a, vel_b = [pick(left[i], right[i]) for i in range(4)]
    field_a, field_b = [pick(left[i], right[i]) for i in (5, 6)]
    energy = pick(energy_l, energy_r)
    total_p = pick(total_l, total_r)
    dot_vb = pick(dot_l, dot_r)
    edge = pick(slow_edge, fast_edge)
    s_dens, s_va, s_vb, s_fa, s_fb, s_dot, s_energy, root = [
        pick(low, high) for low, high in zip(star_l, star_r)
    ]
    way = pick(-1.0, 1.0)
    inner = middle + way * jnp.abs(normal) / root
    ahead = inner > 0.0
    outer = (on_left & (slow_edge > 0.0)) | ~(on_left | (fast_edge > 0.0) | ahead)
    double = (on_left ^ ahead) & ~outer
    d_energy = s_energy + way * root * (s_dot - dbl_dot) * orient
    to_star = jnp.where(outer, 0.0, edge)
    to_double = jnp.where(double, inner, 0.0)
    mass = dens * vel_n
    return (
        mass + to_star * (s_dens - dens),
        mass * vel_n + total_p - normal_sq + to_star * (s_dens * middle - mass),
        mass * vel_a
        - normal * field_a
        + to_star * (s_dens * s_va - dens * vel_a)
        + to_double * (s_dens * (dbl_va - s_va)),
        mass * vel_b
        - normal * field_b
        + to_star * (s_dens * s_vb - dens * vel_b)
        + to_double * (s_dens * (dbl_vb - s_vb)),
        (energy + total_p) * vel_n
        - normal * dot_vb
        + to_star * (s_energy - energy)
        + to_double * (d_energy - s_energy),
        field_a * vel_n - normal * vel_a + to_star * (s_fa - field_a) + to_double * (dbl_fa - s_fa),
        field_b * vel_n - normal * vel_b + to_star * (s_fb - field_b) + to_double * (dbl_fb - s_fb),
    )


def sublane_is(which):
    return lax.broadcasted_iota(jnp.int32, (8, 256), 0) == which


def wrapped(tile, by):
    return (tile + by) % 5 if isinstance(tile, int) else lax.rem(tile + by, 5)


def row_before(load, tile):
    return pltpu.roll(jnp.where(sublane_is(7), load(wrapped(tile, 4)), load(tile)), 1, 0)


def row_after(load, tile):
    return pltpu.roll(jnp.where(sublane_is(0), load(wrapped(tile, 1)), load(tile)), 7, 0)


tangents = ((1, 2), (2, 0), (0, 1))


def cell_pass(state, above, cell, left, plane, tile):
    dens = state[0, plane, tile]
    vel = [state[1 + c, plane, tile] for c in range(3)]
    pres = state[4, plane, tile]
    face = [state[5 + c, plane, tile] for c in range(3)]
    cell[0, plane, tile] = 0.5 * (face[0] + shift_x_up(face[0]))
    field_y = 0.5 * (face[1] + row_after(lambda t: state[6, plane, t], tile))
    field_z = 0.5 * (face[2] + above)
    inv_dens = 1.0 / dens
    sound = gamma_gas * pres * inv_dens
    hydro = pres / (gamma_gas - 1.0) + 0.5 * dens * (
        vel[0] * vel[0] + vel[1] * vel[1] + vel[2] * vel[2]
    )
    for f, value in ((1, field_y), (2, field_z), (3, inv_dens), (4, sound), (5, hydro)):
        cell[f, plane, tile] = value
    members = (dens, *vel, pres, field_y, field_z, inv_dens, sound, hydro)
    for f, value in enumerate(members):
        left[f, plane, tile] = shift_x_down(value)


def flux_pass(direction, state, cell, left_x, flux, plane, tile):
    first, second = tangents[direction]
    members = (
        (state, 0),
        (state, 1 + direction),
        (state, 1 + first),
        (state, 1 + second),
        (state, 4),
        (cell, first),
        (cell, second),
        (cell, 3),
        (cell, 4),
        (cell, 5),
    )
    right = [ref[f, plane, tile] for ref, f in members]
    if direction == 0:
        left = [left_x[f, plane, tile] for f in range(10)]
    elif direction == 1:
        left = [row_before(lambda t, ref=ref, f=f: ref[f, plane, t], tile) for ref, f in members]
    else:
        left = [ref[f, plane - 1, tile] for ref, f in members]
    result = hlld_flux(left, right, state[5 + direction, plane, tile])
    for member in range(7):
        flux[direction, member, plane, tile] = result[member]


def edge_pass(flux, edge, plane, tile):
    flow = flux[1, 6, plane, tile]
    edge[2, plane, tile] = 0.25 * (
        flow
        + shift_x_down(flow)
        - flux[0, 5, plane, tile]
        - row_before(lambda t: flux[0, 5, plane, t], tile)
    )
    edge[0, plane, tile] = 0.25 * (
        flux[2, 6, plane, tile]
        + row_before(lambda t: flux[2, 6, plane, t], tile)
        - flux[1, 5, plane, tile]
        - flux[1, 5, plane - 1, tile]
    )
    flow = flux[2, 5, plane, tile]
    edge[1, plane, tile] = 0.25 * (
        flux[0, 6, plane, tile] + flux[0, 6, plane - 1, tile] - flow - shift_x_down(flow)
    )


def update_pass(state, cell, flux, edge, outs, plane, tile):
    new_dens, new_mom, new_energy, new_face = outs
    own = plane - 1

    def change(slots):
        low = flux[0, slots[0], plane, tile]
        total = shift_x_up(low) - low
        total += row_after(lambda t: flux[1, slots[1], plane, t], tile) - flux[1, slots[1], plane, tile]
        return total + (flux[2, slots[2], plane + 1, tile] - flux[2, slots[2], plane, tile])

    dens = state[0, plane, tile]
    new_dens[own, tile] = dens - time_step * change((0, 0, 0))
    slots = ((1, 3, 2), (2, 1, 3), (3, 2, 1))
    for c in range(3):
        new_mom[c, own, tile] = dens * state[1 + c, plane, tile] - time_step * change(slots[c])
    field = [cell[c, plane, tile] for c in range(3)]
    energy = cell[5, plane, tile] + 0.5 * (
        field[0] * field[0] + field[1] * field[1] + field[2] * field[2]
    )
    new_energy[own, tile] = energy - time_step * change((4, 4, 4))
    low = [edge[c, plane, tile] for c in range(3)]
    above = [edge[c, plane + 1, tile] for c in range(2)]
    new_face[0, own, tile] = state[5, plane, tile] - time_step * (
        row_after(lambda t: edge[2, plane, t], tile) - low[2] - (above[1] - low[1])
    )
    new_face[1, own, tile] = state[6, plane, tile] - time_step * (
        above[0] - low[0] - (shift_x_up(low[2]) - low[2])
    )
    new_face[2, own, tile] = state[7, plane, tile] - time_step * (
        shift_x_up(low[1]) - low[1] - (row_after(lambda t: edge[0, plane, t], tile) - low[0])
    )


def pull_pass(state, phi, outs, plane, tile):
    new_dens, new_mom, new_energy, new_face = outs
    own = plane - 1
    centre = phi[plane, tile]
    load = lambda t: phi[plane, t]
    accel = (
        -0.5 * (shift_x_up(centre) - shift_x_down(centre)),
        -0.5 * (row_after(load, tile) - row_before(load, tile)),
        -0.5 * (phi[plane + 1, tile] - phi[plane - 1, tile]),
    )
    pulled = time_step * state[0, plane, tile]
    work = jnp.zeros_like(centre)
    for c in range(3):
        new_mom[c, own, tile] += pulled * accel[c]
        work += pulled * state[1 + c, plane, tile] * accel[c]
    new_energy[own, tile] += work


def step_kernel(
    rows, cols, dens, vel, pres, face, nat_h, perm_c_h, perm_r_h, eig_z_h, eig_y_h, eig_x_h,
    out_dens, out_mom, out_energy, out_face,
    nat, perm_c, perm_r, eig_z, eig_y, eig_x,
    send_a, recv_a, send_c, recv_c, send_e, recv_e, send_g, recv_g,
    state, cell, left, flux, edge, phi, above_bz, rim_out, rim_in, cap_out, cap_in,
    new_dens, new_mom, new_energy, new_face,
    local_s, over_s, over_r, halo_s, halo_r, ready,
):
    row = lax.axis_index("row")
    col = lax.axis_index("col")
    outs = (new_dens, new_mom, new_energy, new_face)
    barrier = pltpu.get_barrier_semaphore()
    row_up = lax.rem(row + 1, rows)
    row_down = lax.rem(row + rows - 1, rows)
    col_up = lax.rem(col + 1, cols)
    col_down = lax.rem(col + cols - 1, cols)

    def copy(src, dst, send, recv, to_row, to_col):
        return pltpu.make_async_remote_copy(
            src_ref=src, dst_ref=dst, send_sem=send, recv_sem=recv,
            device_id={"row": to_row, "col": to_col}, device_id_type=pl.DeviceIdType.MESH,
        )

    def signal(to_row, to_col):
        pl.semaphore_signal(
            barrier, inc=1, device_id={"row": to_row, "col": to_col},
            device_id_type=pl.DeviceIdType.MESH,
        )

    @pl.loop(1, rows)
    def _(s):
        signal(lax.rem(row + s, rows), col)

    @pl.loop(1, 5)
    def _(s):
        signal(row, lax.rem(col + s, cols))
        signal(row, lax.rem(col + cols - s, cols))

    def pass_on(number, by):
        for step in (by, cols - by):
            pl.semaphore_signal(
                ready.at[number], inc=1, device_id={"row": row, "col": lax.rem(col + step, cols)},
                device_id_type=pl.DeviceIdType.MESH,
            )

    def passed(number):
        pl.semaphore_wait(ready.at[number], 2)

    reads = [
        pltpu.make_async_copy(src, dst, local_s.at[i])
        for i, (src, dst) in enumerate(
            (
                (dens, state.at[0, 1:9, 0:4]),
                (nat_h, nat),
                (vel, state.at[1:4, 1:9, 0:4]),
                (pres, state.at[4, 1:9, 0:4]),
                (face, state.at[5:8, 1:9, 0:4]),
                (perm_c_h, perm_c),
                (perm_r_h, perm_r),
                (eig_z_h, eig_z),
                (eig_y_h, eig_y),
                (eig_x_h, eig_x),
            )
        )
    ]
    writes = [
        pltpu.make_async_copy(src, dst, local_s.at[i])
        for i, (src, dst) in enumerate(
            (
                (new_dens, out_dens),
                (new_face, out_face),
                (new_mom, out_mom),
                (new_energy, out_energy),
            )
        )
    ]
    for one in reads:
        one.start()

    def row_copy(peer, src, dst, number, h):
        at = 2 * number + h
        return copy(src.at[h, peer], dst.at[h, row], over_s.at[at], over_r.at[at], peer, col)

    def col_copy(peer, src, dst, number, h):
        at = 2 * number + h
        return copy(src.at[h, peer], dst.at[h, col], over_s.at[at], over_r.at[at], row, peer)

    def start_row(*over):
        @pl.loop(1, rows)
        def _(s):
            row_copy(lax.rem(row + s, rows), *over).start()

    def start_col(*over):
        @pl.loop(1, cols)
        def _(s):
            col_copy(lax.rem(col + s, cols), *over).start()

    def all_row(src, dst, number, h):
        at, part = 2 * number + h, slice(0, rows - 1)
        return copy(src.at[h, part], dst.at[h, part], over_s.at[at], over_r.at[at], row_up, col)

    def all_col(src, dst, number, h):
        at, part = 2 * number + h, slice(0, cols - 1)
        return copy(src.at[h, part], dst.at[h, part], over_s.at[at], over_r.at[at], row, col_up)

    over_a = (send_a, recv_a, 0)
    over_c = (send_c, recv_c, 1)
    over_e = (send_e, recv_e, 2)
    over_g = (send_g, recv_g, 3)

    def halo(number, src, dst, to_row, to_col):
        return copy(src, dst, halo_s.at[number], halo_r.at[number], to_row, to_col)

    rims = (
        halo(0, rim_out.at[0], rim_in.at[0], row_down, col),
        halo(0, rim_out.at[1], rim_in.at[1], row_up, col),
    )
    rims_all = halo(0, rim_out, rim_in, row_up, col)
    layers = (
        halo(1, state.at[:, 8, 0:4], state.at[:, 0, 0:4], row, col_up),
        halo(2, state.at[:, 1, 0:4], state.at[:, 9, 0:4], row, col_down),
        halo(3, state.at[7, 2, 0:4], above_bz.at[0:4], row, col_down),
    )
    corners = (
        halo(4, state.at[:, 8, 4], state.at[:, 0, 4], row, col_up),
        halo(5, state.at[:, 1, 4], state.at[:, 9, 4], row, col_down),
        halo(6, state.at[7, 2, 4], above_bz.at[4], row, col_down),
    )
    caps = []
    for number, (plane, to_col) in enumerate(((0, col_down), (1, col_up))):
        caps.append(
            (
                lambda peer, n=number, c=to_col: copy(
                    cap_out.at[n, peer], cap_in.at[n, row], halo_s.at[7 + n], halo_r.at[7 + n], peer, c
                ),
                halo(7 + number, cap_out.at[number], cap_in.at[number], row, to_col),
            )
        )

    def cells(low, high, tiles):
        @pl.loop(low, high)
        def _(plane):
            for tile in tiles:
                cell_pass(state, state[7, plane + 1, tile], cell, left, plane, tile)

    def fluxes(direction, low, high, first, last):
        @pl.loop(low, high)
        def _(plane):
            @pl.loop(first, last)
            def _(tile):
                flux_pass(direction, state, cell, left, flux, plane, tile)

    reads[0].wait()
    reads[1].wait()
    spec = mm(state[0, 1:9, 0:4].reshape(256, 256), nat[...])
    for h in range(2):
        for g in range(2):
            parts = [
                spec[32 * z : 32 * z + 32, 128 * g : 128 * g + 128] for z in range(4 * h, 4 * h + 4)
            ]
            for r, part in enumerate(transpose_chunks(parts)):
                send_a[h, 4 * g + r] = part
        recv_a[h, row] = send_a[h, row]
    for one in reads[2:]:
        one.wait()
    for f in range(8):
        rim_out[0, f] = state[f, 1:9, 0, 0, :]
        rim_out[1, f] = state[f, 1:9, 3, 7, :]
    second = state[6, 1:9, 0, 1, :]
    rim_out[0, 8] = second
    rim_out[1, 8] = second

    cells(1, 8, range(3))
    fluxes(0, 1, 4, 0, 3)
    pl.semaphore_wait(barrier, rows - 1 + 8)

    for h in range(2):
        start_row(*over_a, h)
    for one in rims:
        one.start()
    for one in layers:
        one.start()
    pass_on(0, 4)
    fluxes(0, 4, 8, 0, 3)
    rims_all.wait_recv()
    sub = lax.broadcasted_iota(jnp.int32, (8, 256), 0)
    for f in range(8):
        first = rim_in[0, f]
        last = rim_in[1, f]
        second = rim_in[0, 8]
        for k in range(8):
            tile = jnp.where(sub == 0, first[k : k + 1], last[k : k + 1])
            if f == 6:
                tile = jnp.where(sub == 1, second[k : k + 1], tile)
            state[f, k + 1, 4] = tile
    for one in corners:
        one.start()
    passed(0)
    pass_on(1, 8)
    fluxes(1, 1, 8, 1, 3)
    fluxes(2, 2, 8, 0, 3)

    passed(1)
    for h in range(2):
        all_row(*over_a, h).wait_recv()
        spec = mm(nat[...], recv_a[h].reshape(256, 128))
        send_c[h] = spec.reshape(32, 8, 128)
        recv_c[h, col] = send_c[h, col]
        start_col(*over_c, h)
    cells(1, 8, range(3, 5))
    fluxes(0, 1, 8, 3, 5)
    fluxes(2, 2, 8, 3, 5)
    fluxes(1, 1, 8, 3, 5)
    fluxes(1, 1, 8, 0, 1)

    for h in range(2):
        all_col(*over_c, h).wait_recv()
    stacked = []
    for h in range(2):
        low = transpose_chunks([recv_c.at[h][:, y, :] for y in range(4)])
        high = transpose_chunks([recv_c.at[h][:, y, :] for y in range(4, 8)])
        stacked += [side_by_side(*pair) for pair in zip(low, high)]
    full = mm(perm_c[...], jnp.concatenate(stacked, axis=0))
    total = eig_z[...] + (eig_y[pl.ds(col, 1), :] + eig_x[pl.ds(row, 1), :])
    kz = lax.broadcasted_iota(jnp.int32, (256, 256), 0)
    lane = lax.broadcasted_iota(jnp.int32, (256, 256), 1)
    anchor = kz + lane + row + col == 0
    full = full * jnp.where(anchor, 0.0, (coupling / 2.0**24) / jnp.where(anchor, 1.0, total))
    for h in range(2):
        back = mm(perm_r[128 * h : 128 * h + 128], full)
        for g in range(2):
            parts = [back[32 * z : 32 * z + 32, 128 * g : 128 * g + 128] for z in range(4)]
            for y, part in enumerate(transpose_chunks(parts)):
                send_e[h, :, 4 * g + y, :] = part
        recv_e[h, col] = send_e[h, col]
        start_col(*over_e, h)
    for one in (*layers, *corners):
        one.wait_recv()
    cells(0, 1, range(5))
    cells(8, 9, range(5))
    for tile in range(5):
        cell_pass(state, above_bz[tile], cell, left, 9, tile)
    fluxes(0, 8, 10, 0, 5)
    fluxes(0, 0, 1, 0, 5)
    fluxes(1, 8, 10, 0, 5)
    fluxes(1, 0, 1, 0, 5)
    fluxes(2, 8, 10, 0, 5)
    fluxes(2, 1, 2, 0, 5)

    @pl.loop(1, 10)
    def _(plane):
        for tile in range(5):
            edge_pass(flux, edge, plane, tile)

    @pl.loop(1, 9)
    def _(plane):
        for tile in range(4):
            update_pass(state, cell, flux, edge, outs, plane, tile)

    for one in writes[:2]:
        one.start()

    low_tile = lax.broadcasted_iota(jnp.int32, (8, 128), 0) == 7
    chunk = lax.broadcasted_iota(jnp.int32, (8, 128), 1) // 32
    for h in range(2):
        all_col(*over_e, h).wait_recv()
        back = mm(nat[...], recv_e[h].reshape(256, 128))
        tiles = [back[8 * t : 8 * t + 8] for t in range(32)]
        for r in range(8):
            send_g[h, r, :32] = back[32 * r : 32 * r + 32]
            send_g[h, r, 32:] = jnp.where(low_tile, tiles[(4 * r + 31) % 32], tiles[(4 * r + 4) % 32])
        recv_g[h, row] = send_g[h, row]
        start_row(*over_g, h)
        for r in range(8):
            packed = tiles[4 * r + 3 * h]
            for t in range(4):
                if t != 3 * h:
                    shift = 32 * (t - 3 * h) % 128
                    packed = jnp.where(chunk == t, pltpu.roll(tiles[4 * r + t], shift, 1), packed)
            cap_out[h, r] = packed

        @pl.loop(0, rows)
        def _(s, one=caps[h][0]):
            one(lax.rem(row + s, rows)).start()

    def planes_of(parts, rows_each):
        low = transpose_chunks(parts[:4])
        high = transpose_chunks(parts[4:])
        full = jnp.concatenate([side_by_side(*pair) for pair in zip(low, high)], axis=0)
        return mm(full, nat[...])

    for h in range(2):
        all_row(*over_g, h).wait_recv()
        full = planes_of([recv_g[h, r] for r in range(8)], 40)
        phi[1 + 4 * h : 5 + 4 * h] = full.reshape(4, 5, 8, 256)

    def pulls(low, high):
        @pl.loop(low, high)
        def _(plane):
            for tile in range(4):
                pull_pass(state, phi, outs, plane, tile)

    pulls(2, 8)
    for number, plane in ((0, 9), (1, 0)):
        caps[number][1].wait_recv()
        full = planes_of([cap_in[number, r] for r in range(8)], 8)
        phi[plane, 0:4] = full.reshape(4, 8, 256)
    pulls(1, 2)
    pulls(8, 9)
    for one in writes[2:]:
        one.start()
    for h in range(2):
        all_row(*over_a, h).wait_send()
        all_row(*over_g, h).wait_send()
        all_col(*over_c, h).wait_send()
        all_col(*over_e, h).wait_send()
    for one in (rims_all, *layers, *corners, caps[0][1], caps[1][1]):
        one.wait_send()
    for one in writes:
        one.wait()


def write_kernel(*refs):
    sources, targets, sems = refs[:4], refs[4:8], refs[8]
    moves = [pltpu.make_async_copy(s, t, sems.at[i]) for i, (s, t) in enumerate(zip(sources, targets))]
    for one in moves:
        one.start()
    for one in moves:
        one.wait()


def written(*results):
    return pl.pallas_call(
        write_kernel,
        out_shape=tuple(jax.ShapeDtypeStruct(r.shape, r.dtype) for r in results),
        in_specs=[pl.BlockSpec(memory_space=pl.ANY)] * 4,
        out_specs=(pl.BlockSpec(memory_space=pltpu.HBM),) * 4,
        scratch_shapes=[pltpu.SemaphoreType.DMA((4,))],
        compiler_params=pltpu.CompilerParams(vmem_limit_bytes=1024 * 1024),
        name="write",
    )(*results)


def local(density, velocity, pressure, face_field):
    rows = lax.axis_size("row")
    cols = lax.axis_size("col")
    nat, perm_c, perm_r, values = tables(256, 8)
    eig_z = np.ascontiguousarray(np.broadcast_to(values[:, None], (256, 256)), dtype=np.float32)
    eig_y = np.repeat(values.reshape(32, 8), 32, axis=1).astype(np.float32)
    eig_x = np.tile(values.reshape(8, 32), (1, 8)).astype(np.float32)
    dma = pltpu.SemaphoreType.DMA
    f = jnp.float32
    vm = lambda *shape: pltpu.VMEM(shape, f)
    block = (8, 4, 8, 256)
    scalar = jax.ShapeDtypeStruct(block, f)
    vector = jax.ShapeDtypeStruct((3, *block), f)
    results = pl.pallas_call(
        functools.partial(step_kernel, rows, cols),
        out_shape=(scalar, vector, scalar, vector),
        in_specs=[pl.BlockSpec(memory_space=pltpu.HBM)] * 10,
        out_specs=(pl.BlockSpec(memory_space=pl.ANY),) * 4,
        scratch_shapes=[
            vm(256, 256), vm(256, 256), vm(256, 256), vm(256, 256), vm(32, 256), vm(8, 256),
            vm(2, 8, 32, 128), vm(2, 8, 32, 128),
            vm(2, 32, 8, 128), vm(2, 32, 8, 128),
            vm(2, 32, 8, 128), vm(2, 32, 8, 128),
            vm(2, 8, 40, 128), vm(2, 8, 40, 128),
            vm(8, 10, 5, 8, 256), vm(6, 10, 5, 8, 256), vm(10, 10, 5, 8, 256),
            vm(3, 7, 10, 5, 8, 256), vm(3, 10, 5, 8, 256),
            vm(10, 5, 8, 256), vm(5, 8, 256),
            vm(2, 9, 8, 256), vm(2, 9, 8, 256),
            vm(2, 8, 8, 128), vm(2, 8, 8, 128),
            vm(*block), vm(3, *block), vm(*block), vm(3, *block),
            dma((10,)), dma((8,)), dma((8,)), dma((9,)), dma((9,)),
            pltpu.SemaphoreType.REGULAR((2,)),
        ],
        compiler_params=pltpu.CompilerParams(
            collective_id=0, has_side_effects=True, vmem_limit_bytes=40 * 1024 * 1024
        ),
        name="step",
    )(
        *(
            pltpu.with_memory_space_constraint(x, pltpu.HBM)
            for x in (
                density.reshape(block), velocity.reshape(3, *block), pressure.reshape(block),
                face_field.reshape(3, *block), jnp.asarray(nat), jnp.asarray(perm_c),
                jnp.asarray(perm_r), jnp.asarray(eig_z), jnp.asarray(eig_y), jnp.asarray(eig_x),
            )
        )
    )
    results = written(*results)
    return (
        results[0].reshape(density.shape),
        results[1].reshape(velocity.shape),
        results[2].reshape(density.shape),
        results[3].reshape(velocity.shape),
    )


def solution(mesh):
    in_specs = (
        P("col", "row", None),
        P(None, "col", "row", None),
        P("col", "row", None),
        P(None, "col", "row", None),
    )
    out_specs = (
        P("col", "row", None),
        P(None, "col", "row", None),
        P("col", "row", None),
        P(None, "col", "row", None),
    )
    return jax.shard_map(local, mesh=mesh, in_specs=in_specs, out_specs=out_specs, check_vma=False)
```

```python
import functools
import math

import jax
import jax.numpy as jnp
import numpy as np
from jax import lax
from jax.experimental import pallas as pl
from jax.experimental.pallas import tpu as pltpu
from jax.sharding import PartitionSpec as P

gamma_gas = 5.0 / 3.0
time_step = 0.1
coupling = 3.0


def tables(size, chunk):
    index = np.arange(size)
    angle = (index[:, None] * index[None, :] % size) * (2.0 * math.pi / size)
    natural = np.cos(angle) + np.sin(angle)
    order = np.arange(size).reshape(size // chunk, chunk).T.reshape(-1)
    values = 2.0 * np.cos(index * (2.0 * math.pi / size)) - 2.0
    as32 = lambda x: np.ascontiguousarray(x, dtype=np.float32)
    return (as32(natural), as32(natural[:, order]), as32(natural[order, :]), values)


def mm(a, b):
    return lax.dot_general(
        a,
        b,
        (((1,), (0,)), ((), ())),
        precision=lax.Precision.HIGHEST,
        preferred_element_type=jnp.float32,
    )


def transpose_chunks(parts):
    lane = lax.broadcasted_iota(jnp.int32, parts[0].shape, 1)
    for bit, width in ((2, 64), (1, 32)):
        keep = (lane // width) % 2 == 0
        fresh = [None] * 4
        for i in range(4):
            if i & bit:
                continue
            low, high = parts[i], parts[i | bit]
            fresh[i] = jnp.where(keep, low, pltpu.roll(high, width, 1))
            fresh[i | bit] = jnp.where(keep, pltpu.roll(low, 128 - width, 1), high)
        parts = fresh
    return parts


def side_by_side(low, high):
    return jnp.concatenate([low, high], axis=1)


def shift_x_down(x):
    return pltpu.roll(x, 1, 1)


def shift_x_up(x):
    return pltpu.roll(x, 255, 1)


def side_terms(side, normal, normal_sq):
    dens, vel_n, vel_a, vel_b, pres, field_a, field_b, inv_dens, sound, hydro = side
    across = field_a * field_a + field_b * field_b
    magnetic = 0.5 * (normal_sq + across)
    energy = hydro + magnetic
    total_p = pres + magnetic
    dot_vb = vel_n * normal + vel_a * field_a + vel_b * field_b
    along = normal_sq * inv_dens
    across = across * inv_dens
    gap = sound - along - across
    fast_sq = sound + along + across + jnp.sqrt(gap * gap + 4.0 * sound * across)
    return (energy, total_p, dot_vb, fast_sq)


def star_state(side, normal, normal_sq, energy, total_p, dot_vb, relative, mass, edge, middle, star_p):
    dens, vel_n, vel_a, vel_b, pres, field_a, field_b = side[:7]
    edge_gap = edge - middle
    inv_gap = 1.0 / edge_gap
    inv_div = 1.0 / (mass * edge_gap - normal_sq)
    star_dens = mass * inv_gap
    offset = normal * (middle - vel_n) * inv_div
    star_va = vel_a - field_a * offset
    star_vb = vel_b - field_b * offset
    factor = (mass * relative - normal_sq) * inv_div
    star_fa = field_a * factor
    star_fb = field_b * factor
    star_dot = middle * normal + star_va * star_fa + star_vb * star_fb
    star_energy = (
        relative * energy - total_p * vel_n + star_p * middle + normal * (dot_vb - star_dot)
    ) * inv_gap
    return (star_dens, star_va, star_vb, star_fa, star_fb, star_dot, star_energy, jnp.sqrt(star_dens))


def hlld_flux(left, right, normal):
    normal_sq = normal * normal
    energy_l, total_l, dot_l, fast_l = side_terms(left, normal, normal_sq)
    energy_r, total_r, dot_r, fast_r = side_terms(right, normal, normal_sq)
    fastest = jnp.sqrt(0.5 * jnp.maximum(fast_l, fast_r))
    slow_edge = jnp.minimum(left[1], right[1]) - fastest
    fast_edge = jnp.maximum(left[1], right[1]) + fastest
    rel_l = slow_edge - left[1]
    rel_r = fast_edge - right[1]
    mass_l = left[0] * rel_l
    mass_r = right[0] * rel_r
    inv_weight = 1.0 / (mass_r - mass_l)
    middle = (mass_r * right[1] - mass_l * left[1] - total_r + total_l) * inv_weight
    star_p = (
        mass_r * total_l - mass_l * total_r + mass_l * mass_r * (right[1] - left[1])
    ) * inv_weight
    star_l = star_state(
        left, normal, normal_sq, energy_l, total_l, dot_l, rel_l, mass_l, slow_edge, middle, star_p
    )
    star_r = star_state(
        right, normal, normal_sq, energy_r, total_r, dot_r, rel_r, mass_r, fast_edge, middle, star_p
    )
    root_l, root_r = star_l[7], star_r[7]
    orient = jnp.where(normal > 0.0, 1.0, jnp.where(normal < 0.0, -1.0, 0.0))
    inv_sum = 1.0 / (root_l + root_r)
    both = root_l * root_r * orient
    dbl_va = (root_l * star_l[1] + root_r * star_r[1] + (star_r[3] - star_l[3]) * orient) * inv_sum
    dbl_vb = (root_l * star_l[2] + root_r * star_r[2] + (star_r[4] - star_l[4]) * orient) * inv_sum
    dbl_fa = (root_l * star_r[3] + root_r * star_l[3] + both * (star_r[1] - star_l[1])) * inv_sum
    dbl_fb = (root_l * star_r[4] + root_r * star_l[4] + both * (star_r[2] - star_l[2])) * inv_sum
    dbl_dot = middle * normal + dbl_va * dbl_fa + dbl_vb * dbl_fb
    on_left = (middle > 0.0) | (slow_edge > 0.0)

    def pick(low, high):
        return jnp.where(on_left, low, high)

    dens, vel_n, vel_a, vel_b = [pick(left[i], right[i]) for i in range(4)]
    field_a, field_b = [pick(left[i], right[i]) for i in (5, 6)]
    energy = pick(energy_l, energy_r)
    total_p = pick(total_l, total_r)
    dot_vb = pick(dot_l, dot_r)
    edge = pick(slow_edge, fast_edge)
    s_dens, s_va, s_vb, s_fa, s_fb, s_dot, s_energy, root = [
        pick(low, high) for low, high in zip(star_l, star_r)
    ]
    way = pick(-1.0, 1.0)
    inner = middle + way * jnp.abs(normal) / root
    ahead = inner > 0.0
    outer = (on_left & (slow_edge > 0.0)) | ~(on_left | (fast_edge > 0.0) | ahead)
    double = (on_left ^ ahead) & ~outer
    d_energy = s_energy + way * root * (s_dot - dbl_dot) * orient
    to_star = jnp.where(outer, 0.0, edge)
    to_double = jnp.where(double, inner, 0.0)
    mass = dens * vel_n
    return (
        mass + to_star * (s_dens - dens),
        mass * vel_n + total_p - normal_sq + to_star * (s_dens * middle - mass),
        mass * vel_a
        - normal * field_a
        + to_star * (s_dens * s_va - dens * vel_a)
        + to_double * (s_dens * (dbl_va - s_va)),
        mass * vel_b
        - normal * field_b
        + to_star * (s_dens * s_vb - dens * vel_b)
        + to_double * (s_dens * (dbl_vb - s_vb)),
        (energy + total_p) * vel_n
        - normal * dot_vb
        + to_star * (s_energy - energy)
        + to_double * (d_energy - s_energy),
        field_a * vel_n - normal * vel_a + to_star * (s_fa - field_a) + to_double * (dbl_fa - s_fa),
        field_b * vel_n - normal * vel_b + to_star * (s_fb - field_b) + to_double * (dbl_fb - s_fb),
    )


def sublane_is(which):
    return lax.broadcasted_iota(jnp.int32, (8, 256), 0) == which


def wrapped(tile, by):
    return (tile + by) % 5 if isinstance(tile, int) else lax.rem(tile + by, 5)


def row_before(load, tile):
    return pltpu.roll(jnp.where(sublane_is(7), load(wrapped(tile, 4)), load(tile)), 1, 0)


def row_after(load, tile):
    return pltpu.roll(jnp.where(sublane_is(0), load(wrapped(tile, 1)), load(tile)), 7, 0)


tangents = ((1, 2), (2, 0), (0, 1))


def cell_pass(state, above, cell, left, plane, tile):
    dens = state[0, plane, tile]
    vel = [state[1 + c, plane, tile] for c in range(3)]
    pres = state[4, plane, tile]
    face = [state[5 + c, plane, tile] for c in range(3)]
    cell[0, plane, tile] = 0.5 * (face[0] + shift_x_up(face[0]))
    field_y = 0.5 * (face[1] + row_after(lambda t: state[6, plane, t], tile))
    field_z = 0.5 * (face[2] + above)
    inv_dens = 1.0 / dens
    sound = gamma_gas * pres * inv_dens
    hydro = pres / (gamma_gas - 1.0) + 0.5 * dens * (
        vel[0] * vel[0] + vel[1] * vel[1] + vel[2] * vel[2]
    )
    for f, value in ((1, field_y), (2, field_z), (3, inv_dens), (4, sound), (5, hydro)):
        cell[f, plane, tile] = value
    members = (dens, *vel, pres, field_y, field_z, inv_dens, sound, hydro)
    for f, value in enumerate(members):
        left[f, plane, tile] = shift_x_down(value)


def flux_pass(direction, state, cell, left_x, flux, plane, tile):
    first, second = tangents[direction]
    members = (
        (state, 0),
        (state, 1 + direction),
        (state, 1 + first),
        (state, 1 + second),
        (state, 4),
        (cell, first),
        (cell, second),
        (cell, 3),
        (cell, 4),
        (cell, 5),
    )
    right = [ref[f, plane, tile] for ref, f in members]
    if direction == 0:
        left = [left_x[f, plane, tile] for f in range(10)]
    elif direction == 1:
        left = [row_before(lambda t, ref=ref, f=f: ref[f, plane, t], tile) for ref, f in members]
    else:
        left = [ref[f, plane - 1, tile] for ref, f in members]
    result = hlld_flux(left, right, state[5 + direction, plane, tile])
    for member in range(7):
        flux[direction, member, plane, tile] = result[member]


def edge_pass(flux, edge, plane, tile):
    flow = flux[1, 6, plane, tile]
    edge[2, plane, tile] = 0.25 * (
        flow
        + shift_x_down(flow)
        - flux[0, 5, plane, tile]
        - row_before(lambda t: flux[0, 5, plane, t], tile)
    )
    edge[0, plane, tile] = 0.25 * (
        flux[2, 6, plane, tile]
        + row_before(lambda t: flux[2, 6, plane, t], tile)
        - flux[1, 5, plane, tile]
        - flux[1, 5, plane - 1, tile]
    )
    flow = flux[2, 5, plane, tile]
    edge[1, plane, tile] = 0.25 * (
        flux[0, 6, plane, tile] + flux[0, 6, plane - 1, tile] - flow - shift_x_down(flow)
    )


def update_pass(state, cell, flux, edge, outs, plane, tile):
    new_dens, new_mom, new_energy, new_face = outs
    own = plane - 1

    def change(slots):
        low = flux[0, slots[0], plane, tile]
        total = shift_x_up(low) - low
        total += row_after(lambda t: flux[1, slots[1], plane, t], tile) - flux[1, slots[1], plane, tile]
        return total + (flux[2, slots[2], plane + 1, tile] - flux[2, slots[2], plane, tile])

    dens = state[0, plane, tile]
    new_dens[own, tile] = dens - time_step * change((0, 0, 0))
    slots = ((1, 3, 2), (2, 1, 3), (3, 2, 1))
    for c in range(3):
        new_mom[c, own, tile] = dens * state[1 + c, plane, tile] - time_step * change(slots[c])
    field = [cell[c, plane, tile] for c in range(3)]
    energy = cell[5, plane, tile] + 0.5 * (
        field[0] * field[0] + field[1] * field[1] + field[2] * field[2]
    )
    new_energy[own, tile] = energy - time_step * change((4, 4, 4))
    low = [edge[c, plane, tile] for c in range(3)]
    above = [edge[c, plane + 1, tile] for c in range(2)]
    new_face[0, own, tile] = state[5, plane, tile] - time_step * (
        row_after(lambda t: edge[2, plane, t], tile) - low[2] - (above[1] - low[1])
    )
    new_face[1, own, tile] = state[6, plane, tile] - time_step * (
        above[0] - low[0] - (shift_x_up(low[2]) - low[2])
    )
    new_face[2, own, tile] = state[7, plane, tile] - time_step * (
        shift_x_up(low[1]) - low[1] - (row_after(lambda t: edge[0, plane, t], tile) - low[0])
    )


def pull_pass(state, phi, outs, plane, tile):
    new_dens, new_mom, new_energy, new_face = outs
    own = plane - 1
    centre = phi[plane, tile]
    load = lambda t: phi[plane, t]
    accel = (
        -0.5 * (shift_x_up(centre) - shift_x_down(centre)),
        -0.5 * (row_after(load, tile) - row_before(load, tile)),
        -0.5 * (phi[plane + 1, tile] - phi[plane - 1, tile]),
    )
    pulled = time_step * state[0, plane, tile]
    work = jnp.zeros_like(centre)
    for c in range(3):
        new_mom[c, own, tile] += pulled * accel[c]
        work += pulled * state[1 + c, plane, tile] * accel[c]
    new_energy[own, tile] += work


def step_kernel(
    rows, cols, dens, vel, pres, face, nat_h, perm_c_h, perm_r_h, eig_z_h, eig_y_h, eig_x_h,
    out_dens, out_mom, out_energy, out_face,
    nat, perm_c, perm_r, eig_z, eig_y, eig_x,
    send_a, recv_a, send_c, recv_c, send_e, recv_e, send_g, recv_g,
    state, cell, left, flux, edge, phi, above_bz, rim_out, rim_in, cap_out, cap_in,
    new_dens, new_mom, new_energy, new_face,
    local_s, over_s, over_r, halo_s, halo_r, ready,
):
    row = lax.axis_index("row")
    col = lax.axis_index("col")
    outs = (new_dens, new_mom, new_energy, new_face)
    barrier = pltpu.get_barrier_semaphore()
    row_up = lax.rem(row + 1, rows)
    row_down = lax.rem(row + rows - 1, rows)
    col_up = lax.rem(col + 1, cols)
    col_down = lax.rem(col + cols - 1, cols)

    def copy(src, dst, send, recv, to_row, to_col):
        return pltpu.make_async_remote_copy(
            src_ref=src, dst_ref=dst, send_sem=send, recv_sem=recv,
            device_id={"row": to_row, "col": to_col}, device_id_type=pl.DeviceIdType.MESH,
        )

    def signal(to_row, to_col):
        pl.semaphore_signal(
            barrier, inc=1, device_id={"row": to_row, "col": to_col},
            device_id_type=pl.DeviceIdType.MESH,
        )

    @pl.loop(1, rows)
    def _(s):
        signal(lax.rem(row + s, rows), col)

    @pl.loop(1, 5)
    def _(s):
        signal(row, lax.rem(col + s, cols))
        signal(row, lax.rem(col + cols - s, cols))

    def pass_on(number, by):
        for step in (by, cols - by):
            pl.semaphore_signal(
                ready.at[number], inc=1, device_id={"row": row, "col": lax.rem(col + step, cols)},
                device_id_type=pl.DeviceIdType.MESH,
            )

    def passed(number):
        pl.semaphore_wait(ready.at[number], 2)

    reads = [
        pltpu.make_async_copy(src, dst, local_s.at[i])
        for i, (src, dst) in enumerate(
            (
                (dens, state.at[0, 1:9, 0:4]),
                (nat_h, nat),
                (vel, state.at[1:4, 1:9, 0:4]),
                (pres, state.at[4, 1:9, 0:4]),
                (face, state.at[5:8, 1:9, 0:4]),
                (perm_c_h, perm_c),
                (perm_r_h, perm_r),
                (eig_z_h, eig_z),
                (eig_y_h, eig_y),
                (eig_x_h, eig_x),
            )
        )
    ]
    writes = [
        pltpu.make_async_copy(src, dst, local_s.at[i])
        for i, (src, dst) in enumerate(
            (
                (new_dens, out_dens),
                (new_face, out_face),
                (new_mom, out_mom),
                (new_energy, out_energy),
            )
        )
    ]
    for one in reads:
        one.start()

    def row_copy(peer, src, dst, number, h):
        at = 2 * number + h
        return copy(src.at[h, peer], dst.at[h, row], over_s.at[at], over_r.at[at], peer, col)

    def col_copy(peer, src, dst, number, h):
        at = 2 * number + h
        return copy(src.at[h, peer], dst.at[h, col], over_s.at[at], over_r.at[at], row, peer)

    def start_row(*over):
        @pl.loop(1, rows)
        def _(s):
            row_copy(lax.rem(row + s, rows), *over).start()

    def start_col(*over):
        half, quarter = cols // 2, cols // 4

        @pl.loop(0, half - 1)
        def _(i):
            far = quarter + (i + 1) // 2 * (1 - 2 * lax.rem(i, 2))
            col_copy(lax.rem(col + far, cols), *over).start()
            col_copy(lax.rem(col + half + far, cols), *over).start()

        col_copy(lax.rem(col + half, cols), *over).start()

    def all_row(src, dst, number, h):
        at, part = 2 * number + h, slice(0, rows - 1)
        return copy(src.at[h, part], dst.at[h, part], over_s.at[at], over_r.at[at], row_up, col)

    def all_col(src, dst, number, h):
        at, part = 2 * number + h, slice(0, cols - 1)
        return copy(src.at[h, part], dst.at[h, part], over_s.at[at], over_r.at[at], row, col_up)

    over_a = (send_a, recv_a, 0)
    over_c = (send_c, recv_c, 1)
    over_e = (send_e, recv_e, 2)
    over_g = (send_g, recv_g, 3)

    def halo(number, src, dst, to_row, to_col):
        return copy(src, dst, halo_s.at[number], halo_r.at[number], to_row, to_col)

    rims = (
        halo(0, rim_out.at[0], rim_in.at[0], row_down, col),
        halo(0, rim_out.at[1], rim_in.at[1], row_up, col),
    )
    rims_all = halo(0, rim_out, rim_in, row_up, col)
    layers = (
        halo(1, state.at[:, 8, 0:4], state.at[:, 0, 0:4], row, col_up),
        halo(2, state.at[:, 1, 0:4], state.at[:, 9, 0:4], row, col_down),
        halo(3, state.at[7, 2, 0:4], above_bz.at[0:4], row, col_down),
    )
    corners = (
        halo(4, state.at[:, 8, 4], state.at[:, 0, 4], row, col_up),
        halo(5, state.at[:, 1, 4], state.at[:, 9, 4], row, col_down),
        halo(6, state.at[7, 2, 4], above_bz.at[4], row, col_down),
    )
    caps = []
    for number, (plane, to_col) in enumerate(((0, col_down), (1, col_up))):
        caps.append(
            (
                lambda peer, n=number, c=to_col: copy(
                    cap_out.at[n, peer], cap_in.at[n, row], halo_s.at[7 + n], halo_r.at[7 + n], peer, c
                ),
                halo(7 + number, cap_out.at[number], cap_in.at[number], row, to_col),
            )
        )

    def cells(low, high, tiles):
        @pl.loop(low, high)
        def _(plane):
            for tile in tiles:
                cell_pass(state, state[7, plane + 1, tile], cell, left, plane, tile)

    def fluxes(direction, low, high, first, last):
        @pl.loop(low, high)
        def _(plane):
            @pl.loop(first, last)
            def _(tile):
                flux_pass(direction, state, cell, left, flux, plane, tile)

    reads[0].wait()
    reads[1].wait()
    spec = mm(state[0, 1:9, 0:4].reshape(256, 256), nat[...])
    for h in range(2):
        for g in range(2):
            parts = [
                spec[32 * z : 32 * z + 32, 128 * g : 128 * g + 128] for z in range(4 * h, 4 * h + 4)
            ]
            for r, part in enumerate(transpose_chunks(parts)):
                send_a[h, 4 * g + r] = part
        recv_a[h, row] = send_a[h, row]
    pl.semaphore_wait(barrier, rows - 1 + 8)

    for h in range(2):
        start_row(*over_a, h)
    pass_on(0, 4)
    for one in reads[2:]:
        one.wait()
    for f in range(8):
        rim_out[0, f] = state[f, 1:9, 0, 0, :]
        rim_out[1, f] = state[f, 1:9, 3, 7, :]
    second = state[6, 1:9, 0, 1, :]
    rim_out[0, 8] = second
    rim_out[1, 8] = second

    for one in rims:
        one.start()

    cells(1, 8, range(3))
    passed(0)
    pass_on(1, 8)
    for one in layers:
        one.start()
    fluxes(0, 1, 5, 0, 3)
    rims_all.wait_recv()
    sub = lax.broadcasted_iota(jnp.int32, (8, 256), 0)
    for f in range(8):
        first = rim_in[0, f]
        last = rim_in[1, f]
        second = rim_in[0, 8]
        for k in range(8):
            tile = jnp.where(sub == 0, first[k : k + 1], last[k : k + 1])
            if f == 6:
                tile = jnp.where(sub == 1, second[k : k + 1], tile)
            state[f, k + 1, 4] = tile
    for one in corners:
        one.start()
    total = eig_z[...] + (eig_y[pl.ds(col, 1), :] + eig_x[pl.ds(row, 1), :])
    kz = lax.broadcasted_iota(jnp.int32, (256, 256), 0)
    lane = lax.broadcasted_iota(jnp.int32, (256, 256), 1)
    anchor = kz + lane + row + col == 0
    eig_z[...] = jnp.where(anchor, 0.0, (coupling / 2.0**24) / jnp.where(anchor, 1.0, total))

    fluxes(0, 5, 8, 0, 3)

    passed(1)
    for h in range(2):
        all_row(*over_a, h).wait_recv()
        spec = mm(nat[...], recv_a[h].reshape(256, 128))
        send_c[h] = spec.reshape(32, 8, 128)
        recv_c[h, col] = send_c[h, col]
        start_col(*over_c, h)
    fluxes(1, 1, 8, 1, 3)
    fluxes(2, 2, 8, 0, 3)
    cells(1, 8, range(3, 5))
    fluxes(0, 1, 8, 3, 5)
    fluxes(2, 2, 8, 3, 5)

    for h in range(2):
        all_col(*over_c, h).wait_recv()
    stacked = []
    for h in range(2):
        low = transpose_chunks([recv_c.at[h][:, y, :] for y in range(4)])
        high = transpose_chunks([recv_c.at[h][:, y, :] for y in range(4, 8)])
        stacked += [side_by_side(*pair) for pair in zip(low, high)]
    full = mm(perm_c[...], jnp.concatenate(stacked, axis=0))
    full = full * eig_z[...]
    for h in range(2):
        back = mm(perm_r[128 * h : 128 * h + 128], full)
        for g in range(2):
            parts = [back[32 * z : 32 * z + 32, 128 * g : 128 * g + 128] for z in range(4)]
            for y, part in enumerate(transpose_chunks(parts)):
                send_e[h, :, 4 * g + y, :] = part
        recv_e[h, col] = send_e[h, col]
        start_col(*over_e, h)
    fluxes(1, 1, 8, 3, 5)
    fluxes(1, 1, 8, 0, 1)
    for one in (*layers, *corners):
        one.wait_recv()
    cells(0, 1, range(5))
    cells(8, 9, range(5))
    for tile in range(5):
        cell_pass(state, above_bz[tile], cell, left, 9, tile)
    fluxes(0, 8, 10, 0, 5)
    fluxes(0, 0, 1, 0, 5)
    fluxes(1, 8, 10, 0, 5)
    fluxes(1, 0, 1, 0, 5)

    low_tile = lax.broadcasted_iota(jnp.int32, (8, 128), 0) == 7
    chunk = lax.broadcasted_iota(jnp.int32, (8, 128), 1) // 32
    for h in range(2):
        all_col(*over_e, h).wait_recv()
        back = mm(nat[...], recv_e[h].reshape(256, 128))
        tiles = [back[8 * t : 8 * t + 8] for t in range(32)]
        for r in range(8):
            send_g[h, r, :32] = back[32 * r : 32 * r + 32]
            send_g[h, r, 32:] = jnp.where(low_tile, tiles[(4 * r + 31) % 32], tiles[(4 * r + 4) % 32])
        recv_g[h, row] = send_g[h, row]
        start_row(*over_g, h)
        for r in range(8):
            packed = tiles[4 * r + 3 * h]
            for t in range(4):
                if t != 3 * h:
                    shift = 32 * (t - 3 * h) % 128
                    packed = jnp.where(chunk == t, pltpu.roll(tiles[4 * r + t], shift, 1), packed)
            cap_out[h, r] = packed

        @pl.loop(0, rows)
        def _(s, one=caps[h][0]):
            one(lax.rem(row + s, rows)).start()

    def pulls(low, high):
        @pl.loop(low, high)
        def _(plane):
            for tile in range(4):
                pull_pass(state, phi, outs, plane, tile)

    def planes_of(parts, rows_each):
        low = transpose_chunks(parts[:4])
        high = transpose_chunks(parts[4:])
        full = jnp.concatenate([side_by_side(*pair) for pair in zip(low, high)], axis=0)
        return mm(full, nat[...])

    fluxes(2, 8, 10, 0, 5)
    fluxes(2, 1, 2, 0, 5)

    @pl.loop(1, 10)
    def _(plane):
        for tile in range(5):
            edge_pass(flux, edge, plane, tile)

    @pl.loop(1, 9)
    def _(plane):
        for tile in range(4):
            update_pass(state, cell, flux, edge, outs, plane, tile)

    for one in writes[:2]:
        one.start()

    for h in range(2):
        all_row(*over_g, h).wait_recv()
        full = planes_of([recv_g[h, r] for r in range(8)], 40)
        phi[1 + 4 * h : 5 + 4 * h] = full.reshape(4, 5, 8, 256)
        if h == 0:
            pulls(2, 4)

    pulls(4, 8)
    for number, plane in ((0, 9), (1, 0)):
        caps[number][1].wait_recv()
        full = planes_of([cap_in[number, r] for r in range(8)], 8)
        phi[plane, 0:4] = full.reshape(4, 8, 256)
    pulls(1, 2)
    pulls(8, 9)
    for one in writes[2:]:
        one.start()
    for h in range(2):
        all_row(*over_a, h).wait_send()
        all_row(*over_g, h).wait_send()
        all_col(*over_c, h).wait_send()
        all_col(*over_e, h).wait_send()
    for one in (rims_all, *layers, *corners, caps[0][1], caps[1][1]):
        one.wait_send()
    for one in writes:
        one.wait()


def write_kernel(*refs):
    sources, targets, sems = refs[:4], refs[4:8], refs[8]
    moves = [pltpu.make_async_copy(s, t, sems.at[i]) for i, (s, t) in enumerate(zip(sources, targets))]
    for one in moves:
        one.start()
    for one in moves:
        one.wait()


def written(*results):
    return pl.pallas_call(
        write_kernel,
        out_shape=tuple(jax.ShapeDtypeStruct(r.shape, r.dtype) for r in results),
        in_specs=[pl.BlockSpec(memory_space=pl.ANY)] * 4,
        out_specs=(pl.BlockSpec(memory_space=pltpu.HBM),) * 4,
        scratch_shapes=[pltpu.SemaphoreType.DMA((4,))],
        compiler_params=pltpu.CompilerParams(vmem_limit_bytes=1024 * 1024),
        name="write",
    )(*results)


def local(density, velocity, pressure, face_field):
    rows = lax.axis_size("row")
    cols = lax.axis_size("col")
    nat, perm_c, perm_r, values = tables(256, 8)
    eig_z = np.ascontiguousarray(np.broadcast_to(values[:, None], (256, 256)), dtype=np.float32)
    eig_y = np.repeat(values.reshape(32, 8), 32, axis=1).astype(np.float32)
    eig_x = np.tile(values.reshape(8, 32), (1, 8)).astype(np.float32)
    dma = pltpu.SemaphoreType.DMA
    f = jnp.float32
    vm = lambda *shape: pltpu.VMEM(shape, f)
    block = (8, 4, 8, 256)
    scalar = jax.ShapeDtypeStruct(block, f)
    vector = jax.ShapeDtypeStruct((3, *block), f)
    results = pl.pallas_call(
        functools.partial(step_kernel, rows, cols),
        out_shape=(scalar, vector, scalar, vector),
        in_specs=[pl.BlockSpec(memory_space=pltpu.HBM)] * 10,
        out_specs=(pl.BlockSpec(memory_space=pl.ANY),) * 4,
        scratch_shapes=[
            vm(256, 256), vm(256, 256), vm(256, 256), vm(256, 256), vm(32, 256), vm(8, 256),
            vm(2, 8, 32, 128), vm(2, 8, 32, 128),
            vm(2, 32, 8, 128), vm(2, 32, 8, 128),
            vm(2, 32, 8, 128), vm(2, 32, 8, 128),
            vm(2, 8, 40, 128), vm(2, 8, 40, 128),
            vm(8, 10, 5, 8, 256), vm(6, 10, 5, 8, 256), vm(10, 10, 5, 8, 256),
            vm(3, 7, 10, 5, 8, 256), vm(3, 10, 5, 8, 256),
            vm(10, 5, 8, 256), vm(5, 8, 256),
            vm(2, 9, 8, 256), vm(2, 9, 8, 256),
            vm(2, 8, 8, 128), vm(2, 8, 8, 128),
            vm(*block), vm(3, *block), vm(*block), vm(3, *block),
            dma((10,)), dma((8,)), dma((8,)), dma((9,)), dma((9,)),
            pltpu.SemaphoreType.REGULAR((2,)),
        ],
        compiler_params=pltpu.CompilerParams(
            collective_id=0, has_side_effects=True, vmem_limit_bytes=40 * 1024 * 1024
        ),
        name="step",
    )(
        *(
            pltpu.with_memory_space_constraint(x, pltpu.HBM)
            for x in (
                density.reshape(block), velocity.reshape(3, *block), pressure.reshape(block),
                face_field.reshape(3, *block), jnp.asarray(nat), jnp.asarray(perm_c),
                jnp.asarray(perm_r), jnp.asarray(eig_z), jnp.asarray(eig_y), jnp.asarray(eig_x),
            )
        )
    )
    results = written(*results)
    return (
        results[0].reshape(density.shape),
        results[1].reshape(velocity.shape),
        results[2].reshape(density.shape),
        results[3].reshape(velocity.shape),
    )


def solution(mesh):
    in_specs = (
        P("col", "row", None),
        P(None, "col", "row", None),
        P("col", "row", None),
        P(None, "col", "row", None),
    )
    out_specs = (
        P("col", "row", None),
        P(None, "col", "row", None),
        P("col", "row", None),
        P(None, "col", "row", None),
    )
    return jax.shard_map(local, mesh=mesh, in_specs=in_specs, out_specs=out_specs, check_vma=False)
```

```python
import functools
import math

import jax
import jax.numpy as jnp
import numpy as np
from jax import lax
from jax.experimental import pallas as pl
from jax.experimental.pallas import tpu as pltpu
from jax.sharding import PartitionSpec as P

gamma_gas = 5.0 / 3.0
time_step = 0.1
coupling = 3.0


def tables(size, chunk):
    index = np.arange(size)
    angle = (index[:, None] * index[None, :] % size) * (2.0 * math.pi / size)
    natural = np.cos(angle) + np.sin(angle)
    order = np.arange(size).reshape(size // chunk, chunk).T.reshape(-1)
    values = 2.0 * np.cos(index * (2.0 * math.pi / size)) - 2.0
    as32 = lambda x: np.ascontiguousarray(x, dtype=np.float32)
    return (as32(natural), as32(natural[:, order]), as32(natural[order, :]), values)


def mm(a, b):
    return lax.dot_general(
        a,
        b,
        (((1,), (0,)), ((), ())),
        precision=lax.Precision.HIGHEST,
        preferred_element_type=jnp.float32,
    )


def transpose_chunks(parts):
    lane = lax.broadcasted_iota(jnp.int32, parts[0].shape, 1)
    for bit, width in ((2, 64), (1, 32)):
        keep = (lane // width) % 2 == 0
        fresh = [None] * 4
        for i in range(4):
            if i & bit:
                continue
            low, high = parts[i], parts[i | bit]
            fresh[i] = jnp.where(keep, low, pltpu.roll(high, width, 1))
            fresh[i | bit] = jnp.where(keep, pltpu.roll(low, 128 - width, 1), high)
        parts = fresh
    return parts


def side_by_side(low, high):
    return jnp.concatenate([low, high], axis=1)


def shift_x_down(x):
    return pltpu.roll(x, 1, 1)


def shift_x_up(x):
    return pltpu.roll(x, 255, 1)


def side_terms(side, normal, normal_sq):
    dens, vel_n, vel_a, vel_b, pres, field_a, field_b, inv_dens, sound, hydro = side
    across = field_a * field_a + field_b * field_b
    magnetic = 0.5 * (normal_sq + across)
    energy = hydro + magnetic
    total_p = pres + magnetic
    dot_vb = vel_n * normal + vel_a * field_a + vel_b * field_b
    along = normal_sq * inv_dens
    across = across * inv_dens
    gap = sound - along - across
    fast_sq = sound + along + across + jnp.sqrt(gap * gap + 4.0 * sound * across)
    return (energy, total_p, dot_vb, fast_sq)


def star_state(side, normal, normal_sq, energy, total_p, dot_vb, relative, mass, edge, middle, star_p):
    dens, vel_n, vel_a, vel_b, pres, field_a, field_b = side[:7]
    edge_gap = edge - middle
    inv_gap = 1.0 / edge_gap
    inv_div = 1.0 / (mass * edge_gap - normal_sq)
    star_dens = mass * inv_gap
    offset = normal * (middle - vel_n) * inv_div
    star_va = vel_a - field_a * offset
    star_vb = vel_b - field_b * offset
    factor = (mass * relative - normal_sq) * inv_div
    star_fa = field_a * factor
    star_fb = field_b * factor
    star_dot = middle * normal + star_va * star_fa + star_vb * star_fb
    star_energy = (
        relative * energy - total_p * vel_n + star_p * middle + normal * (dot_vb - star_dot)
    ) * inv_gap
    return (star_dens, star_va, star_vb, star_fa, star_fb, star_dot, star_energy, jnp.sqrt(star_dens))


def hlld_flux(left, right, normal):
    normal_sq = normal * normal
    energy_l, total_l, dot_l, fast_l = side_terms(left, normal, normal_sq)
    energy_r, total_r, dot_r, fast_r = side_terms(right, normal, normal_sq)
    fastest = jnp.sqrt(0.5 * jnp.maximum(fast_l, fast_r))
    slow_edge = jnp.minimum(left[1], right[1]) - fastest
    fast_edge = jnp.maximum(left[1], right[1]) + fastest
    rel_l = slow_edge - left[1]
    rel_r = fast_edge - right[1]
    mass_l = left[0] * rel_l
    mass_r = right[0] * rel_r
    inv_weight = 1.0 / (mass_r - mass_l)
    middle = (mass_r * right[1] - mass_l * left[1] - total_r + total_l) * inv_weight
    star_p = (
        mass_r * total_l - mass_l * total_r + mass_l * mass_r * (right[1] - left[1])
    ) * inv_weight
    star_l = star_state(
        left, normal, normal_sq, energy_l, total_l, dot_l, rel_l, mass_l, slow_edge, middle, star_p
    )
    star_r = star_state(
        right, normal, normal_sq, energy_r, total_r, dot_r, rel_r, mass_r, fast_edge, middle, star_p
    )
    root_l, root_r = star_l[7], star_r[7]
    orient = jnp.where(normal > 0.0, 1.0, jnp.where(normal < 0.0, -1.0, 0.0))
    inv_sum = 1.0 / (root_l + root_r)
    both = root_l * root_r * orient
    dbl_va = (root_l * star_l[1] + root_r * star_r[1] + (star_r[3] - star_l[3]) * orient) * inv_sum
    dbl_vb = (root_l * star_l[2] + root_r * star_r[2] + (star_r[4] - star_l[4]) * orient) * inv_sum
    dbl_fa = (root_l * star_r[3] + root_r * star_l[3] + both * (star_r[1] - star_l[1])) * inv_sum
    dbl_fb = (root_l * star_r[4] + root_r * star_l[4] + both * (star_r[2] - star_l[2])) * inv_sum
    dbl_dot = middle * normal + dbl_va * dbl_fa + dbl_vb * dbl_fb
    on_left = (middle > 0.0) | (slow_edge > 0.0)

    def pick(low, high):
        return jnp.where(on_left, low, high)

    dens, vel_n, vel_a, vel_b = [pick(left[i], right[i]) for i in range(4)]
    field_a, field_b = [pick(left[i], right[i]) for i in (5, 6)]
    energy = pick(energy_l, energy_r)
    total_p = pick(total_l, total_r)
    dot_vb = pick(dot_l, dot_r)
    edge = pick(slow_edge, fast_edge)
    s_dens, s_va, s_vb, s_fa, s_fb, s_dot, s_energy, root = [
        pick(low, high) for low, high in zip(star_l, star_r)
    ]
    way = pick(-1.0, 1.0)
    inner = middle + way * jnp.abs(normal) / root
    ahead = inner > 0.0
    outer = (on_left & (slow_edge > 0.0)) | ~(on_left | (fast_edge > 0.0) | ahead)
    double = (on_left ^ ahead) & ~outer
    d_energy = s_energy + way * root * (s_dot - dbl_dot) * orient
    to_star = jnp.where(outer, 0.0, edge)
    to_double = jnp.where(double, inner, 0.0)
    mass = dens * vel_n
    return (
        mass + to_star * (s_dens - dens),
        mass * vel_n + total_p - normal_sq + to_star * (s_dens * middle - mass),
        mass * vel_a
        - normal * field_a
        + to_star * (s_dens * s_va - dens * vel_a)
        + to_double * (s_dens * (dbl_va - s_va)),
        mass * vel_b
        - normal * field_b
        + to_star * (s_dens * s_vb - dens * vel_b)
        + to_double * (s_dens * (dbl_vb - s_vb)),
        (energy + total_p) * vel_n
        - normal * dot_vb
        + to_star * (s_energy - energy)
        + to_double * (d_energy - s_energy),
        field_a * vel_n - normal * vel_a + to_star * (s_fa - field_a) + to_double * (dbl_fa - s_fa),
        field_b * vel_n - normal * vel_b + to_star * (s_fb - field_b) + to_double * (dbl_fb - s_fb),
    )


def sublane_is(which):
    return lax.broadcasted_iota(jnp.int32, (8, 256), 0) == which


def wrapped(tile, by):
    return (tile + by) % 5 if isinstance(tile, int) else lax.rem(tile + by, 5)


def row_before(load, tile):
    return pltpu.roll(jnp.where(sublane_is(7), load(wrapped(tile, 4)), load(tile)), 1, 0)


def row_after(load, tile):
    return pltpu.roll(jnp.where(sublane_is(0), load(wrapped(tile, 1)), load(tile)), 7, 0)


tangents = ((1, 2), (2, 0), (0, 1))


def cell_pass(state, above, cell, left, plane, tile):
    dens = state[0, plane, tile]
    vel = [state[1 + c, plane, tile] for c in range(3)]
    pres = state[4, plane, tile]
    face = [state[5 + c, plane, tile] for c in range(3)]
    cell[0, plane, tile] = 0.5 * (face[0] + shift_x_up(face[0]))
    field_y = 0.5 * (face[1] + row_after(lambda t: state[6, plane, t], tile))
    field_z = 0.5 * (face[2] + above)
    inv_dens = 1.0 / dens
    sound = gamma_gas * pres * inv_dens
    hydro = pres / (gamma_gas - 1.0) + 0.5 * dens * (
        vel[0] * vel[0] + vel[1] * vel[1] + vel[2] * vel[2]
    )
    for f, value in ((1, field_y), (2, field_z), (3, inv_dens), (4, sound), (5, hydro)):
        cell[f, plane, tile] = value
    members = (dens, *vel, pres, field_y, field_z, inv_dens, sound, hydro)
    for f, value in enumerate(members):
        left[f, plane, tile] = shift_x_down(value)


def flux_pass(direction, state, cell, left_x, flux, plane, tile):
    first, second = tangents[direction]
    members = (
        (state, 0),
        (state, 1 + direction),
        (state, 1 + first),
        (state, 1 + second),
        (state, 4),
        (cell, first),
        (cell, second),
        (cell, 3),
        (cell, 4),
        (cell, 5),
    )
    right = [ref[f, plane, tile] for ref, f in members]
    if direction == 0:
        left = [left_x[f, plane, tile] for f in range(10)]
    elif direction == 1:
        left = [row_before(lambda t, ref=ref, f=f: ref[f, plane, t], tile) for ref, f in members]
    else:
        left = [ref[f, plane - 1, tile] for ref, f in members]
    result = hlld_flux(left, right, state[5 + direction, plane, tile])
    for member in range(7):
        flux[direction, member, plane, tile] = result[member]


def edge_pass(flux, edge, plane, tile):
    flow = flux[1, 6, plane, tile]
    edge[2, plane, tile] = 0.25 * (
        flow
        + shift_x_down(flow)
        - flux[0, 5, plane, tile]
        - row_before(lambda t: flux[0, 5, plane, t], tile)
    )
    edge[0, plane, tile] = 0.25 * (
        flux[2, 6, plane, tile]
        + row_before(lambda t: flux[2, 6, plane, t], tile)
        - flux[1, 5, plane, tile]
        - flux[1, 5, plane - 1, tile]
    )
    flow = flux[2, 5, plane, tile]
    edge[1, plane, tile] = 0.25 * (
        flux[0, 6, plane, tile] + flux[0, 6, plane - 1, tile] - flow - shift_x_down(flow)
    )


def update_pass(state, cell, flux, edge, outs, plane, tile):
    new_dens, new_mom, new_energy, new_face = outs
    own = plane - 1

    def change(slots):
        low = flux[0, slots[0], plane, tile]
        total = shift_x_up(low) - low
        total += row_after(lambda t: flux[1, slots[1], plane, t], tile) - flux[1, slots[1], plane, tile]
        return total + (flux[2, slots[2], plane + 1, tile] - flux[2, slots[2], plane, tile])

    dens = state[0, plane, tile]
    new_dens[own, tile] = dens - time_step * change((0, 0, 0))
    slots = ((1, 3, 2), (2, 1, 3), (3, 2, 1))
    for c in range(3):
        new_mom[c, own, tile] = dens * state[1 + c, plane, tile] - time_step * change(slots[c])
    field = [cell[c, plane, tile] for c in range(3)]
    energy = cell[5, plane, tile] + 0.5 * (
        field[0] * field[0] + field[1] * field[1] + field[2] * field[2]
    )
    new_energy[own, tile] = energy - time_step * change((4, 4, 4))
    low = [edge[c, plane, tile] for c in range(3)]
    above = [edge[c, plane + 1, tile] for c in range(2)]
    new_face[0, own, tile] = state[5, plane, tile] - time_step * (
        row_after(lambda t: edge[2, plane, t], tile) - low[2] - (above[1] - low[1])
    )
    new_face[1, own, tile] = state[6, plane, tile] - time_step * (
        above[0] - low[0] - (shift_x_up(low[2]) - low[2])
    )
    new_face[2, own, tile] = state[7, plane, tile] - time_step * (
        shift_x_up(low[1]) - low[1] - (row_after(lambda t: edge[0, plane, t], tile) - low[0])
    )


def pull_pass(state, phi, outs, plane, tile):
    new_dens, new_mom, new_energy, new_face = outs
    own = plane - 1
    centre = phi[plane, tile]
    load = lambda t: phi[plane, t]
    accel = (
        -0.5 * (shift_x_up(centre) - shift_x_down(centre)),
        -0.5 * (row_after(load, tile) - row_before(load, tile)),
        -0.5 * (phi[plane + 1, tile] - phi[plane - 1, tile]),
    )
    pulled = time_step * state[0, plane, tile]
    work = jnp.zeros_like(centre)
    for c in range(3):
        new_mom[c, own, tile] += pulled * accel[c]
        work += pulled * state[1 + c, plane, tile] * accel[c]
    new_energy[own, tile] += work


def step_kernel(
    rows, cols, dens, vel, pres, face, nat_h, perm_c_h, perm_r_h, eig_z_h, eig_y_h, eig_x_h,
    out_dens, out_mom, out_energy, out_face,
    nat, perm_c, perm_r, eig_z, eig_y, eig_x,
    send_a, recv_a, send_c, recv_c, send_e, recv_e, send_g, recv_g,
    state, cell, left, flux, edge, phi, above_bz, rim_out, rim_in, cap_out, cap_in,
    new_dens, new_mom, new_energy, new_face,
    local_s, over_s, over_r, halo_s, halo_r, ready,
):
    row = lax.axis_index("row")
    col = lax.axis_index("col")
    outs = (new_dens, new_mom, new_energy, new_face)
    barrier = pltpu.get_barrier_semaphore()
    row_up = lax.rem(row + 1, rows)
    row_down = lax.rem(row + rows - 1, rows)
    col_up = lax.rem(col + 1, cols)
    col_down = lax.rem(col + cols - 1, cols)

    def copy(src, dst, send, recv, to_row, to_col):
        return pltpu.make_async_remote_copy(
            src_ref=src, dst_ref=dst, send_sem=send, recv_sem=recv,
            device_id={"row": to_row, "col": to_col}, device_id_type=pl.DeviceIdType.MESH,
        )

    def signal(to_row, to_col):
        pl.semaphore_signal(
            barrier, inc=1, device_id={"row": to_row, "col": to_col},
            device_id_type=pl.DeviceIdType.MESH,
        )

    @pl.loop(1, rows)
    def _(s):
        signal(lax.rem(row + s, rows), col)

    @pl.loop(1, 5)
    def _(s):
        signal(row, lax.rem(col + s, cols))
        signal(row, lax.rem(col + cols - s, cols))

    def pass_on(number, by):
        for step in (by, cols - by):
            pl.semaphore_signal(
                ready.at[number], inc=1, device_id={"row": row, "col": lax.rem(col + step, cols)},
                device_id_type=pl.DeviceIdType.MESH,
            )

    def passed(number):
        pl.semaphore_wait(ready.at[number], 2)

    reads = [
        pltpu.make_async_copy(src, dst, local_s.at[i])
        for i, (src, dst) in enumerate(
            (
                (dens, state.at[0, 1:9, 0:4]),
                (nat_h, nat),
                (vel, state.at[1:4, 1:9, 0:4]),
                (pres, state.at[4, 1:9, 0:4]),
                (face, state.at[5:8, 1:9, 0:4]),
                (perm_c_h, perm_c),
                (perm_r_h, perm_r),
                (eig_z_h, eig_z),
                (eig_y_h, eig_y),
                (eig_x_h, eig_x),
            )
        )
    ]
    writes = [
        pltpu.make_async_copy(src, dst, local_s.at[i])
        for i, (src, dst) in enumerate(
            (
                (new_dens, out_dens),
                (new_face, out_face),
                (new_mom, out_mom),
                (new_energy, out_energy),
            )
        )
    ]
    for one in reads[:2]:
        one.start()

    def row_copy(peer, src, dst, number, h):
        at = 2 * number + h
        return copy(src.at[h, peer], dst.at[h, row], over_s.at[at], over_r.at[at], peer, col)

    def col_copy(peer, src, dst, number, h):
        at = 2 * number + h
        return copy(src.at[h, peer], dst.at[h, col], over_s.at[at], over_r.at[at], row, peer)

    def start_row(*over):
        @pl.loop(1, rows)
        def _(s):
            row_copy(lax.rem(row + s, rows), *over).start()

    def start_col(*over):
        half, quarter = cols // 2, cols // 4

        @pl.loop(0, half - 1)
        def _(i):
            far = quarter + (i + 1) // 2 * (1 - 2 * lax.rem(i, 2))
            col_copy(lax.rem(col + far, cols), *over).start()
            col_copy(lax.rem(col + half + far, cols), *over).start()

        col_copy(lax.rem(col + half, cols), *over).start()

    def all_row(src, dst, number, h):
        at, part = 2 * number + h, slice(0, rows - 1)
        return copy(src.at[h, part], dst.at[h, part], over_s.at[at], over_r.at[at], row_up, col)

    def all_col(src, dst, number, h):
        at, part = 2 * number + h, slice(0, cols - 1)
        return copy(src.at[h, part], dst.at[h, part], over_s.at[at], over_r.at[at], row, col_up)

    over_a = (send_a, recv_a, 0)
    over_c = (send_c, recv_c, 1)
    over_e = (send_e, recv_e, 2)
    over_g = (send_g, recv_g, 3)

    def halo(number, src, dst, to_row, to_col):
        return copy(src, dst, halo_s.at[number], halo_r.at[number], to_row, to_col)

    rims = (
        halo(0, rim_out.at[0], rim_in.at[0], row_down, col),
        halo(0, rim_out.at[1], rim_in.at[1], row_up, col),
    )
    rims_all = halo(0, rim_out, rim_in, row_up, col)
    layers = (
        halo(1, state.at[:, 8, 0:4], state.at[:, 0, 0:4], row, col_up),
        halo(2, state.at[:, 1, 0:4], state.at[:, 9, 0:4], row, col_down),
        halo(3, state.at[7, 2, 0:4], above_bz.at[0:4], row, col_down),
    )
    corners = (
        halo(4, state.at[:, 8, 4], state.at[:, 0, 4], row, col_up),
        halo(5, state.at[:, 1, 4], state.at[:, 9, 4], row, col_down),
        halo(6, state.at[7, 2, 4], above_bz.at[4], row, col_down),
    )
    caps = []
    for number, (plane, to_col) in enumerate(((0, col_down), (1, col_up))):
        caps.append(
            (
                lambda peer, n=number, c=to_col: copy(
                    cap_out.at[n, peer], cap_in.at[n, row], halo_s.at[7 + n], halo_r.at[7 + n], peer, c
                ),
                halo(7 + number, cap_out.at[number], cap_in.at[number], row, to_col),
            )
        )

    def cells(low, high, tiles):
        @pl.loop(low, high)
        def _(plane):
            for tile in tiles:
                cell_pass(state, state[7, plane + 1, tile], cell, left, plane, tile)

    def fluxes(direction, low, high, first, last):
        @pl.loop(low, high)
        def _(plane):
            @pl.loop(first, last)
            def _(tile):
                flux_pass(direction, state, cell, left, flux, plane, tile)

    for one in reads[:2]:
        one.wait()
    for one in reads[2:]:
        one.start()
    spec = mm(state[0, 1:9, 0:4].reshape(256, 256), nat[...])
    for h in range(2):
        for g in range(2):
            parts = [
                spec[32 * z : 32 * z + 32, 128 * g : 128 * g + 128] for z in range(4 * h, 4 * h + 4)
            ]
            for r, part in enumerate(transpose_chunks(parts)):
                send_a[h, 4 * g + r] = part
        recv_a[h, row] = send_a[h, row]
    pl.semaphore_wait(barrier, rows - 1 + 8)

    for h in range(2):
        start_row(*over_a, h)
    pass_on(0, 4)
    for one in reads[2:]:
        one.wait()
    for f in range(8):
        rim_out[0, f] = state[f, 1:9, 0, 0, :]
        rim_out[1, f] = state[f, 1:9, 3, 7, :]
    second = state[6, 1:9, 0, 1, :]
    rim_out[0, 8] = second
    rim_out[1, 8] = second

    for one in rims:
        one.start()

    cells(1, 8, range(3))
    passed(0)
    pass_on(1, 8)
    for one in layers:
        one.start()
    fluxes(0, 1, 5, 0, 3)
    rims_all.wait_recv()
    sub = lax.broadcasted_iota(jnp.int32, (8, 256), 0)
    for f in range(8):
        first = rim_in[0, f]
        last = rim_in[1, f]
        second = rim_in[0, 8]
        for k in range(8):
            tile = jnp.where(sub == 0, first[k : k + 1], last[k : k + 1])
            if f == 6:
                tile = jnp.where(sub == 1, second[k : k + 1], tile)
            state[f, k + 1, 4] = tile
    for one in corners:
        one.start()
    total = eig_z[...] + (eig_y[pl.ds(col, 1), :] + eig_x[pl.ds(row, 1), :])
    kz = lax.broadcasted_iota(jnp.int32, (256, 256), 0)
    lane = lax.broadcasted_iota(jnp.int32, (256, 256), 1)
    anchor = kz + lane + row + col == 0
    eig_z[...] = jnp.where(anchor, 0.0, (coupling / 2.0**24) / jnp.where(anchor, 1.0, total))

    fluxes(0, 5, 8, 0, 3)

    passed(1)
    for h in range(2):
        all_row(*over_a, h).wait_recv()
        spec = mm(nat[...], recv_a[h].reshape(256, 128))
        send_c[h] = spec.reshape(32, 8, 128)
        recv_c[h, col] = send_c[h, col]
        start_col(*over_c, h)
    fluxes(1, 1, 8, 1, 3)
    fluxes(2, 2, 8, 0, 3)
    cells(1, 8, range(3, 5))
    fluxes(0, 1, 8, 3, 5)
    fluxes(2, 2, 8, 3, 5)

    for h in range(2):
        all_col(*over_c, h).wait_recv()
    stacked = []
    for h in range(2):
        low = transpose_chunks([recv_c.at[h][:, y, :] for y in range(4)])
        high = transpose_chunks([recv_c.at[h][:, y, :] for y in range(4, 8)])
        stacked += [side_by_side(*pair) for pair in zip(low, high)]
    full = mm(perm_c[...], jnp.concatenate(stacked, axis=0))
    full = full * eig_z[...]
    for h in range(2):
        back = mm(perm_r[128 * h : 128 * h + 128], full)
        for g in range(2):
            parts = [back[32 * z : 32 * z + 32, 128 * g : 128 * g + 128] for z in range(4)]
            for y, part in enumerate(transpose_chunks(parts)):
                send_e[h, :, 4 * g + y, :] = part
        recv_e[h, col] = send_e[h, col]
        start_col(*over_e, h)
    fluxes(1, 1, 8, 3, 5)
    fluxes(1, 1, 8, 0, 1)
    for one in (*layers, *corners):
        one.wait_recv()
    cells(0, 1, range(5))
    cells(8, 9, range(5))
    for tile in range(5):
        cell_pass(state, above_bz[tile], cell, left, 9, tile)
    fluxes(0, 8, 10, 0, 5)
    fluxes(0, 0, 1, 0, 5)
    fluxes(1, 8, 10, 0, 5)
    fluxes(1, 0, 1, 0, 5)
    fluxes(2, 8, 10, 0, 5)
    fluxes(2, 1, 2, 0, 5)

    @pl.loop(1, 10)
    def _(plane):
        for tile in range(5):
            edge_pass(flux, edge, plane, tile)


    low_tile = lax.broadcasted_iota(jnp.int32, (8, 128), 0) == 7
    chunk = lax.broadcasted_iota(jnp.int32, (8, 128), 1) // 32
    for h in range(2):
        all_col(*over_e, h).wait_recv()
        back = mm(nat[...], recv_e[h].reshape(256, 128))
        tiles = [back[8 * t : 8 * t + 8] for t in range(32)]
        for r in range(8):
            send_g[h, r, :32] = back[32 * r : 32 * r + 32]
            send_g[h, r, 32:] = jnp.where(low_tile, tiles[(4 * r + 31) % 32], tiles[(4 * r + 4) % 32])
        recv_g[h, row] = send_g[h, row]
        start_row(*over_g, h)
        for r in range(8):
            packed = tiles[4 * r + 3 * h]
            for t in range(4):
                if t != 3 * h:
                    shift = 32 * (t - 3 * h) % 128
                    packed = jnp.where(chunk == t, pltpu.roll(tiles[4 * r + t], shift, 1), packed)
            cap_out[h, r] = packed

        @pl.loop(0, rows)
        def _(s, one=caps[h][0]):
            one(lax.rem(row + s, rows)).start()

    def pulls(low, high):
        @pl.loop(low, high)
        def _(plane):
            for tile in range(4):
                pull_pass(state, phi, outs, plane, tile)

    def planes_of(parts, rows_each):
        low = transpose_chunks(parts[:4])
        high = transpose_chunks(parts[4:])
        full = jnp.concatenate([side_by_side(*pair) for pair in zip(low, high)], axis=0)
        return mm(full, nat[...])

    @pl.loop(1, 9)
    def _(plane):
        for tile in range(4):
            update_pass(state, cell, flux, edge, outs, plane, tile)

    for one in writes[:2]:
        one.start()

    for h in range(2):
        all_row(*over_g, h).wait_recv()
        full = planes_of([recv_g[h, r] for r in range(8)], 40)
        phi[1 + 4 * h : 5 + 4 * h] = full.reshape(4, 5, 8, 256)
        if h == 0:
            pulls(2, 4)

    pulls(4, 8)
    for number, plane in ((0, 9), (1, 0)):
        caps[number][1].wait_recv()
        full = planes_of([cap_in[number, r] for r in range(8)], 8)
        phi[plane, 0:4] = full.reshape(4, 8, 256)
    pulls(1, 2)
    pulls(8, 9)
    for one in writes[2:]:
        one.start()
    for h in range(2):
        all_row(*over_a, h).wait_send()
        all_row(*over_g, h).wait_send()
        all_col(*over_c, h).wait_send()
        all_col(*over_e, h).wait_send()
    for one in (rims_all, *layers, *corners, caps[0][1], caps[1][1]):
        one.wait_send()
    for one in writes:
        one.wait()


def write_kernel(*refs):
    sources, targets, sems = refs[:4], refs[4:8], refs[8]
    moves = [pltpu.make_async_copy(s, t, sems.at[i]) for i, (s, t) in enumerate(zip(sources, targets))]
    for one in moves:
        one.start()
    for one in moves:
        one.wait()


def written(*results):
    return pl.pallas_call(
        write_kernel,
        out_shape=tuple(jax.ShapeDtypeStruct(r.shape, r.dtype) for r in results),
        in_specs=[pl.BlockSpec(memory_space=pl.ANY)] * 4,
        out_specs=(pl.BlockSpec(memory_space=pltpu.HBM),) * 4,
        scratch_shapes=[pltpu.SemaphoreType.DMA((4,))],
        compiler_params=pltpu.CompilerParams(vmem_limit_bytes=1024 * 1024),
        name="write",
    )(*results)


def local(density, velocity, pressure, face_field):
    rows = lax.axis_size("row")
    cols = lax.axis_size("col")
    nat, perm_c, perm_r, values = tables(256, 8)
    eig_z = np.ascontiguousarray(np.broadcast_to(values[:, None], (256, 256)), dtype=np.float32)
    eig_y = np.repeat(values.reshape(32, 8), 32, axis=1).astype(np.float32)
    eig_x = np.tile(values.reshape(8, 32), (1, 8)).astype(np.float32)
    dma = pltpu.SemaphoreType.DMA
    f = jnp.float32
    vm = lambda *shape: pltpu.VMEM(shape, f)
    block = (8, 4, 8, 256)
    scalar = jax.ShapeDtypeStruct(block, f)
    vector = jax.ShapeDtypeStruct((3, *block), f)
    results = pl.pallas_call(
        functools.partial(step_kernel, rows, cols),
        out_shape=(scalar, vector, scalar, vector),
        in_specs=[pl.BlockSpec(memory_space=pltpu.HBM)] * 10,
        out_specs=(pl.BlockSpec(memory_space=pl.ANY),) * 4,
        scratch_shapes=[
            vm(256, 256), vm(256, 256), vm(256, 256), vm(256, 256), vm(32, 256), vm(8, 256),
            vm(2, 8, 32, 128), vm(2, 8, 32, 128),
            vm(2, 32, 8, 128), vm(2, 32, 8, 128),
            vm(2, 32, 8, 128), vm(2, 32, 8, 128),
            vm(2, 8, 40, 128), vm(2, 8, 40, 128),
            vm(8, 10, 5, 8, 256), vm(6, 10, 5, 8, 256), vm(10, 10, 5, 8, 256),
            vm(3, 7, 10, 5, 8, 256), vm(3, 10, 5, 8, 256),
            vm(10, 5, 8, 256), vm(5, 8, 256),
            vm(2, 9, 8, 256), vm(2, 9, 8, 256),
            vm(2, 8, 8, 128), vm(2, 8, 8, 128),
            vm(*block), vm(3, *block), vm(*block), vm(3, *block),
            dma((10,)), dma((8,)), dma((8,)), dma((9,)), dma((9,)),
            pltpu.SemaphoreType.REGULAR((2,)),
        ],
        compiler_params=pltpu.CompilerParams(
            collective_id=0, has_side_effects=True, vmem_limit_bytes=40 * 1024 * 1024
        ),
        name="step",
    )(
        *(
            pltpu.with_memory_space_constraint(x, pltpu.HBM)
            for x in (
                density.reshape(block), velocity.reshape(3, *block), pressure.reshape(block),
                face_field.reshape(3, *block), jnp.asarray(nat), jnp.asarray(perm_c),
                jnp.asarray(perm_r), jnp.asarray(eig_z), jnp.asarray(eig_y), jnp.asarray(eig_x),
            )
        )
    )
    results = written(*results)
    return (
        results[0].reshape(density.shape),
        results[1].reshape(velocity.shape),
        results[2].reshape(density.shape),
        results[3].reshape(velocity.shape),
    )


def solution(mesh):
    in_specs = (
        P("col", "row", None),
        P(None, "col", "row", None),
        P("col", "row", None),
        P(None, "col", "row", None),
    )
    out_specs = (
        P("col", "row", None),
        P(None, "col", "row", None),
        P("col", "row", None),
        P(None, "col", "row", None),
    )
    return jax.shard_map(local, mesh=mesh, in_specs=in_specs, out_specs=out_specs, check_vma=False)
```
